8 devices in a mesh: data: 1 (over z), tp: 2 (over y), ep: 4 (over x, core).
Axes of the slice: x: 2, y: 2, z: 1, core: 2. Of those that a mesh axis runs over, the one named last changes fastest.
Arguments:
- tokens_a: bfloat16 [1024, 1536], P(('data', 'ep', 'tp'))
- tokens_b: bfloat16 [1024, 1536], P(('data', 'ep', 'tp'))
- experts_a: int32 [1024, 6], P(('data', 'ep', 'tp'))
- experts_b: int32 [1024, 6], P(('data', 'ep', 'tp'))
- gates_a: float32 [1024, 6], P(('data', 'ep', 'tp'))
- gates_b: float32 [1024, 6], P(('data', 'ep', 'tp'))
- slots_a: int32 [1024, 6], P(('data', 'ep', 'tp'))
- slots_b: int32 [1024, 6], P(('data', 'ep', 'tp'))
- shared_w1: bfloat16 [1536, 1024], P(None, 'tp')
- shared_w3: bfloat16 [1536, 1024], P(None, 'tp')
- shared_w2: bfloat16 [1024, 1536], P('tp')
- routed_w1: bfloat16 [64, 1536, 512], P('ep')
- routed_w3: bfloat16 [64, 1536, 512], P('ep')
- routed_w2: bfloat16 [64, 512, 1536], P('ep')
Outputs:
- output 1: bfloat16 [1024, 1536], P(('data', 'ep', 'tp'))
- output 2: bfloat16 [1024, 1536], P(('data', 'ep', 'tp'))
All inputs are finite; a program needn't handle non-finite values.
Results may differ from the reference program's by a relative error of at most 0.00605838.
Values are sent between devices in bfloat16 or wider.
A program may use at most 1 GiB of HBM per device.

```python
import jax
import jax.numpy as jnp
from jax import lax

TOK_DEV = 128
TP_SIZE = 2
EP_SIZE = 4
MODEL_DIM = 1536
EXPERTS = 64
TOP_K = 6
EXPERT_FF = 512
SHARED_FF = 1024
CAPACITY = 24

GROUP_DEVS = TP_SIZE * EP_SIZE
GROUP_TOK = GROUP_DEVS * TOK_DEV


def draw_routing(key):
    key_base, key_rank, key_tie = jax.random.split(key, 3)
    base = jax.random.randint(key_base, (GROUP_TOK, EXPERTS), 0, 64)
    rank_of = jax.random.permutation(key_rank, EXPERTS)
    favoured = jnp.where((rank_of >= 1) & (rank_of <= EXPERTS // 8), 6, 0)
    forced = jnp.where(rank_of == 0, 4096, 0)
    tok_ids = jnp.arange(GROUP_TOK)
    head_tok = (tok_ids % TOK_DEV) < CAPACITY
    cover = jnp.where(tok_ids[:, None] == jnp.arange(EXPERTS)[None, :], 4096, 0)
    score = base + favoured[None, :] + jnp.where(head_tok[:, None], forced[None, :], 0) + cover
    tie_rank = jax.random.permutation(key_tie, jnp.broadcast_to(jnp.arange(EXPERTS), (GROUP_TOK, EXPERTS)), axis=1, independent=True)
    chosen = lax.top_k(score * EXPERTS + tie_rank, TOP_K)[1]
    per_dev = chosen.reshape(GROUP_DEVS, TOK_DEV * TOP_K)
    one_hot = (per_dev[:, :, None] == jnp.arange(EXPERTS)[None, None, :]).astype(jnp.int32)
    earlier = jnp.cumsum(one_hot, axis=1) - one_hot
    position = jnp.sum(earlier * one_hot, axis=2)
    slots = jnp.where(position < CAPACITY, position, -1).reshape(GROUP_TOK, TOP_K)
    return chosen.astype(jnp.int32), slots.astype(jnp.int32)


def setup_inputs(seed: int = 0, part: int = 0) -> dict:
    key = jax.random.key(seed)
    part_keys = jax.random.split(jax.random.fold_in(key, part), 6)
    weight_keys = jax.random.split(key, 6)
    tokens_a = jax.random.normal(part_keys[0], (GROUP_TOK, MODEL_DIM), jnp.float32).astype(jnp.bfloat16)
    tokens_b = jax.random.normal(part_keys[1], (GROUP_TOK, MODEL_DIM), jnp.float32).astype(jnp.bfloat16)
    experts_a, slots_a = draw_routing(part_keys[2])
    experts_b, slots_b = draw_routing(part_keys[3])
    gates_a = jax.random.uniform(part_keys[4], (GROUP_TOK, TOP_K), jnp.float32, 0.5, 1.5) * TOP_K ** -0.5
    gates_b = jax.random.uniform(part_keys[5], (GROUP_TOK, TOP_K), jnp.float32, 0.5, 1.5) * TOP_K ** -0.5
    shared_w1 = (jax.random.normal(weight_keys[0], (MODEL_DIM, SHARED_FF), jnp.float32) * MODEL_DIM ** -0.5).astype(jnp.bfloat16)
    shared_w3 = (jax.random.normal(weight_keys[1], (MODEL_DIM, SHARED_FF), jnp.float32) * MODEL_DIM ** -0.5).astype(jnp.bfloat16)
    shared_w2 = (jax.random.normal(weight_keys[2], (SHARED_FF, MODEL_DIM), jnp.float32) * SHARED_FF ** -0.5).astype(jnp.bfloat16)
    routed_w1 = (jax.random.normal(weight_keys[3], (EXPERTS, MODEL_DIM, EXPERT_FF), jnp.float32) * MODEL_DIM ** -0.5).astype(jnp.bfloat16)
    routed_w3 = (jax.random.normal(weight_keys[4], (EXPERTS, MODEL_DIM, EXPERT_FF), jnp.float32) * MODEL_DIM ** -0.5).astype(jnp.bfloat16)
    routed_w2 = (jax.random.normal(weight_keys[5], (EXPERTS, EXPERT_FF, MODEL_DIM), jnp.float32) * EXPERT_FF ** -0.5).astype(jnp.bfloat16)
    return {'tokens_a': tokens_a, 'tokens_b': tokens_b, 'experts_a': experts_a, 'experts_b': experts_b, 'gates_a': gates_a, 'gates_b': gates_b, 'slots_a': slots_a, 'slots_b': slots_b, 'shared_w1': shared_w1, 'shared_w3': shared_w3, 'shared_w2': shared_w2, 'routed_w1': routed_w1, 'routed_w3': routed_w3, 'routed_w2': routed_w2}


def swiglu_rows(rows, w_in, w_gate, w_out):
    proj_in = jnp.dot(rows, w_in, preferred_element_type=jnp.float32)
    proj_gate = jnp.dot(rows, w_gate, preferred_element_type=jnp.float32)
    hidden = (jax.nn.silu(proj_in) * proj_gate).astype(jnp.bfloat16)
    return jnp.dot(hidden, w_out, preferred_element_type=jnp.float32)


def shared_expert(tokens, shared_w1, shared_w3, shared_w2):
    blocks = tokens.reshape(GROUP_DEVS, TOK_DEV, MODEL_DIM)
    result = lax.map(lambda token_block: swiglu_rows(token_block, shared_w1, shared_w3, shared_w2), blocks)
    return result.reshape(GROUP_TOK, MODEL_DIM)


def routed_experts(tokens, experts, gates, slots, routed_w1, routed_w3, routed_w2):
    tok_dev = tokens.reshape(GROUP_DEVS, TOK_DEV, MODEL_DIM).astype(jnp.float32)
    expert_dev = experts.reshape(GROUP_DEVS, TOK_DEV, TOP_K)
    slot_dev = slots.reshape(GROUP_DEVS, TOK_DEV, TOP_K)
    gate_dev = gates.reshape(GROUP_DEVS, TOK_DEV, TOP_K)
    slot_range = jnp.arange(CAPACITY)

    def one_expert(routed_acc, step_in):
        w_in, w_gate, w_out, expert = step_in
        hits = ((expert_dev == expert)[..., None] & (slot_dev[..., None] == slot_range)).astype(jnp.float32)
        place_mat = jnp.sum(hits, axis=2)
        gate_mat = jnp.sum(hits * gate_dev[..., None], axis=2)
        buffer_rows = jnp.einsum('ntc,ntd->ncd', place_mat, tok_dev).astype(jnp.bfloat16)
        expert_out = swiglu_rows(buffer_rows.reshape(GROUP_DEVS * CAPACITY, MODEL_DIM), w_in, w_gate, w_out).astype(jnp.bfloat16)
        expert_out = expert_out.reshape(GROUP_DEVS, CAPACITY, MODEL_DIM).astype(jnp.float32)
        return routed_acc + jnp.einsum('ntc,ncd->ntd', gate_mat, expert_out), None

    start_acc = jnp.zeros((GROUP_DEVS, TOK_DEV, MODEL_DIM), jnp.float32)
    routed_acc, unused = lax.scan(one_expert, start_acc, (routed_w1, routed_w3, routed_w2, jnp.arange(EXPERTS)))
    return routed_acc.reshape(GROUP_TOK, MODEL_DIM)


def one_microbatch(tokens, experts, gates, slots, shared_w1, shared_w3, shared_w2, routed_w1, routed_w3, routed_w2):
    shared_out = shared_expert(tokens, shared_w1, shared_w3, shared_w2)
    routed_out = routed_experts(tokens, experts, gates, slots, routed_w1, routed_w3, routed_w2)
    return (tokens.astype(jnp.float32) + shared_out + routed_out).astype(jnp.bfloat16)


def reference(tokens_a, tokens_b, experts_a, experts_b, gates_a, gates_b, slots_a, slots_b, shared_w1, shared_w3, shared_w2, routed_w1, routed_w3, routed_w2):
    out_a = one_microbatch(tokens_a, experts_a, gates_a, slots_a, shared_w1, shared_w3, shared_w2, routed_w1, routed_w3, routed_w2)
    out_b = one_microbatch(tokens_b, experts_b, gates_b, slots_b, shared_w1, shared_w3, shared_w2, routed_w1, routed_w3, routed_w2)
    return (out_a, out_b)
```

```python
import functools

import jax
import jax.numpy as jnp
from jax import lax
from jax.experimental import pallas as pl
from jax.experimental.pallas import tpu as pltpu
from jax.sharding import PartitionSpec as P

MESH = pl.DeviceIdType.MESH
F32, BF16 = jnp.float32, jnp.bfloat16

TOK = 128
DIM = 1536
FF = 512
TOPK = 6
CAP = 24
NE = 16
PAIR = 2 * CAP
ROWS = 2 * PAIR
ALLR = NE * PAIR
CH = 512
NCH = DIM // CH
NRING = 3
W2G = 4
BF16_MAX = 3.3895313892515355e38


def dot(a, b):
    return jnp.dot(a, b, preferred_element_type=F32)


def kernel(tok_a, tok_b, e_a, s_a, e_b, s_b, g_a, g_b, sw1, sw3, sw2, rw1, rw3, rw2,
           out_a, out_b,
           ring, w2r, sw13, sw2v, tok, ytok, rowbuf, hid, rbuf, pmat, g3,
           sendr, sendl, recvr, recvl, xs, xr, acc, hso, hyo, hsi, ost, mi, mg,
           loc_sem, ring_sem, w2_sem, snd, rcv, credit):
    tp = lax.axis_index('tp')
    ep = lax.axis_index('ep')
    core = lax.rem(ep, 2)
    first = ep * NE
    dev_d = {'ep': ep + 1 - 2 * core}
    dev_x = {'ep': lax.rem(ep + 2, 4)}
    dev_y = {'tp': 1 - tp}
    toks, ids, gates = (tok_a, tok_b), (e_a, s_a, e_b, s_b), (g_a, g_b)
    outs = (out_a, out_b)

    def remote(src, dst, sem, dev):
        return pltpu.make_async_remote_copy(src_ref=src, dst_ref=dst, send_sem=snd.at[sem], recv_sem=rcv.at[sem],
                                            device_id=dev, device_id_type=MESH)

    own = [pltpu.make_async_copy(toks[m], tok.at[2 * m, pl.ds(0, TOK)], loc_sem.at[m]) for m in range(2)]
    own += [pltpu.make_async_copy(ids[i], mi.at[0, i], loc_sem.at[2 + i]) for i in range(4)]
    own += [pltpu.make_async_copy(gates[m], mg.at[0, m], loc_sem.at[6 + m]) for m in range(2)]
    shared = [pltpu.make_async_copy(sw1, sw13.at[0], loc_sem.at[8]),
              pltpu.make_async_copy(sw3, sw13.at[1], loc_sem.at[9]),
              pltpu.make_async_copy(sw2, sw2v.at[0], loc_sem.at[10])]

    def ring_copies(expert, slot):
        return (pltpu.make_async_copy(rw1.at[expert], ring.at[slot, 0], ring_sem.at[slot, 0]),
                pltpu.make_async_copy(rw3.at[expert], ring.at[slot, 1], ring_sem.at[slot, 1]))

    def w2_copy(i):
        return pltpu.make_async_copy(rw2.at[pl.ds(i * W2G, W2G)], w2r.at[pl.ds(i * W2G, W2G)], w2_sem.at[i])

    for c in own:
        c.start()
    shared[0].start()
    shared[1].start()
    for q in range(NRING):
        for c in ring_copies(q, q):
            c.start()
    for i in range(NE // W2G):
        w2_copy(i).start()
    shared[2].start()

    barrier = pltpu.get_barrier_semaphore()
    for dev in (dev_d, dev_x, dev_y):
        pl.semaphore_signal(barrier, inc=1, device_id=dev, device_id_type=MESH)
    pl.semaphore_wait(barrier, 3)

    d_meta = [remote(ids[i], mi.at[1, i], i, dev_d) for i in range(4)]
    d_meta += [remote(gates[m], mg.at[1, m], 4 + m, dev_d) for m in range(2)]
    x_meta = [remote(ids[i], mi.at[2, i], 6 + i, dev_x) for i in range(4)]
    x_meta += [remote(gates[m], mg.at[2, m], 10 + m, dev_x) for m in range(2)]
    f_meta = [remote(mi.at[2], mi.at[3], 12, dev_d), remote(mg.at[2], mg.at[3], 13, dev_d)]
    x_tok = [remote(toks[m], tok.at[2 * m + 1, pl.ds(0, TOK)], 14 + m, dev_x) for m in range(2)]
    d_tok = [remote(toks[m], tok.at[2 * m, pl.ds(TOK, TOK)], 16 + m, dev_d) for m in range(2)]
    f_tok = [remote(tok.at[2 * m + 1, pl.ds(0, TOK)], tok.at[2 * m + 1, pl.ds(TOK, TOK)], 18 + m, dev_d)
             for m in range(2)]
    y_tok = [remote(toks[m], ytok.at[pl.ds(m * TOK, TOK)], 20 + m, dev_y) for m in range(2)]
    half = pl.ds(pl.multiple_of(core * (FF // 2), FF // 2), FF // 2)
    y_w2 = remote(sw2.at[half], sw2v.at[1, half], 22, dev_y)
    f_w2 = remote(sw2v.at[1, half], sw2v.at[1, half], 23, dev_d)
    y_hid = remote(hyo, hsi, 24, dev_y)

    def d_rem(c):
        return remote(sendr.at[c], recvr.at[c], 25 + c, dev_d)

    def d_loc(c):
        return remote(sendl.at[c], recvl.at[c], 25 + NCH + c, dev_d)

    def x_part(m, c):
        return remote(xs.at[c], xr.at[m * NCH + c], 25 + 2 * NCH + m * NCH + c, dev_x)

    for c in x_meta + x_tok[:1] + d_meta + d_tok + x_tok[1:] + y_tok + [y_w2]:
        c.start()

    def swiglu(rows, w1, w3):
        p1 = dot(rows, w1)
        p3 = dot(rows, w3)
        return (jax.nn.silu(p1) * p3).astype(BF16)

    def build(m, pair):
        for pos in range(2):
            src = 2 * pair + pos
            slot = mi[src, 2 * m + 1]
            el = mi[src, 2 * m] - first
            ok = (slot >= 0) & (el >= 0) & (el < NE)
            rid = jnp.where(ok, el * PAIR + pos * CAP + slot, -1)
            g = mg[src, m]

            def block(b, _, pos=pos, rid=rid, g=g):
                at = pl.ds(pl.multiple_of(b * 128, 128), 128)
                row = lax.broadcasted_iota(jnp.int32, (128, TOK), 0) + b * 128
                hit = jnp.zeros((128, TOK), F32)
                gt = jnp.zeros((128, TOK), F32)
                for j in range(TOPK):
                    same = row == rid[j:j + 1, :]
                    hit = jnp.where(same, 1.0, hit)
                    gt = jnp.where(same, g[j:j + 1, :], gt)
                pmat[at, pos * TOK:(pos + 1) * TOK] = hit.astype(BF16)
                gg = gt.T
                hi = jnp.minimum(gg, BF16_MAX).astype(BF16)
                r1 = gg - hi.astype(F32)
                mid = r1.astype(BF16)
                lo = (r1 - mid.astype(F32)).astype(BF16)
                for k, v in enumerate((hi, mid, lo)):
                    g3[pair, k, pos * TOK:(pos + 1) * TOK, at] = v
                return 0
            lax.fori_loop(0, ALLR // 128, block, 0)

    def dispatch(m, pair):
        def group(b, _):
            p = pmat[pl.ds(pl.multiple_of(b * 4 * PAIR, 4 * PAIR), 4 * PAIR), :]
            rows = dot(p, tok[2 * m + pair]).astype(BF16)
            for i in range(4):
                rowbuf[b * 4 + i, pair * PAIR:(pair + 1) * PAIR, :] = rows[i * PAIR:(i + 1) * PAIR]
            return 0
        lax.fori_loop(0, NE // 4, group, 0)

    def phase1(m):
        def step(e, _):
            it = m * NE + e
            q = lax.rem(it, NRING)
            for c in ring_copies(e, q):
                c.wait()
            hid[e] = swiglu(rowbuf[e], ring[q, 0], ring[q, 1])

            @pl.when(it + NRING < 2 * NE)
            def _():
                for c in ring_copies(lax.rem(it + NRING, NE), q):
                    c.start()
            return 0
        lax.fori_loop(0, NE, step, 0)

    def combine(pair):
        r = rbuf[pair]
        return dot(g3[pair, 0], r) + dot(g3[pair, 1], r) + dot(g3[pair, 2], r)

    def phase2(m):
        def chunk(c, _):
            cols = pl.ds(pl.multiple_of(c * CH, CH), CH)

            def step(e, _):
                r = dot(hid[e], w2r[e, :, cols]).astype(BF16)
                at = pl.ds(pl.multiple_of(e * PAIR, PAIR), PAIR)
                rbuf[0, at, :] = r[:PAIR]
                rbuf[1, at, :] = r[PAIR:]
                return 0
            lax.fori_loop(0, NE, step, 0)
            if m == 1:
                d_rem(c).wait_send()
                d_loc(c).wait_send()
                x_part(0, c).wait_send()
            part = combine(1)
            sendr[c] = part[TOK:]
            d_rem(c).start()
            xs[c] = part[:TOK]
            part = combine(0)
            sendl[c] = part[TOK:]
            d_loc(c).start()
            acc[m * NCH + c] = part[:TOK]
            d_rem(c).wait_recv()
            xs[c] = xs[c] + recvr[c]
            x_part(m, c).start()
            return 0
        lax.fori_loop(0, NCH, chunk, 0)

    def take_local(m):
        def chunk(c, _):
            d_loc(c).wait_recv()
            acc[m * NCH + c] = acc[m * NCH + c] + recvl[c]
            return 0
        lax.fori_loop(0, NCH, chunk, 0)

    for c in own:
        c.wait()
    shared[0].wait()
    shared[1].wait()
    for m in range(2):
        hso[m] = swiglu(tok[2 * m, :TOK], sw13[0], sw13[1])
    for c in d_meta + d_tok:
        c.wait_recv()
    build(0, 0)
    dispatch(0, 0)
    for c in x_meta:
        c.wait_recv()
    for c in f_meta:
        c.start()
    for c in f_meta:
        c.wait_recv()
    build(0, 1)
    x_tok[0].wait_recv()
    f_tok[0].start()
    f_tok[0].wait_recv()
    dispatch(0, 1)

    phase1(0)
    x_tok[1].wait_recv()
    f_tok[1].start()
    for i in range(NE // W2G):
        w2_copy(i).wait()
    phase2(0)
    for c in y_tok:
        c.wait_recv()
    hyo[0] = swiglu(ytok[:TOK], sw13[0], sw13[1])
    hyo[1] = swiglu(ytok[TOK:], sw13[0], sw13[1])
    y_hid.start()
    take_local(0)
    pl.semaphore_signal(credit, inc=1, device_id=dev_d, device_id_type=MESH)

    build(1, 0)
    dispatch(1, 0)
    build(1, 1)
    f_tok[1].wait_recv()
    dispatch(1, 1)
    phase1(1)
    y_w2.wait_recv()
    f_w2.start()
    pl.semaphore_wait(credit, 1)
    phase2(1)
    take_local(1)

    shared[2].wait()
    f_w2.wait_recv()
    y_hid.wait_recv()
    for m in range(2):
        def base(c, _, m=m):
            cols = pl.ds(pl.multiple_of(c * CH, CH), CH)
            s = dot(hso[m], sw2v[0, :, cols]) + dot(hsi[m], sw2v[1, :, cols])
            acc[m * NCH + c] = acc[m * NCH + c] + s + tok[2 * m, pl.ds(0, TOK), cols].astype(F32)
            return 0
        lax.fori_loop(0, NCH, base, 0)
    put = [pltpu.make_async_copy(ost.at[m], outs[m], loc_sem.at[11 + m]) for m in range(2)]
    for m in range(2):
        def last(c, _, m=m):
            cols = pl.ds(pl.multiple_of(c * CH, CH), CH)
            x_part(m, c).wait_recv()
            ost[m, :, cols] = (acc[m * NCH + c] + xr[m * NCH + c]).astype(BF16)
            return 0
        lax.fori_loop(0, NCH, last, 0)
        put[m].start()

    for c in x_meta + x_tok + d_meta + d_tok + f_meta + f_tok + y_tok + [y_w2, f_w2, y_hid]:
        c.wait_send()
    for c in range(NCH):
        d_rem(c).wait_send()
        d_loc(c).wait_send()
        x_part(1, c).wait_send()
    for c in put:
        c.wait()


def solution(mesh):
    tok_spec = P(('data', 'ep', 'tp'), None)
    in_specs = (tok_spec,) * 8 + (P(None, 'tp'), P(None, 'tp'), P('tp', None), P('ep', None, None), P('ep', None, None), P('ep', None, None))
    nsem = 25 + 4 * NCH
    scratch = [
        pltpu.VMEM((NRING, 2, DIM, FF), BF16),
        pltpu.VMEM((NE, FF, DIM), BF16),
        pltpu.VMEM((2, DIM, FF), BF16),
        pltpu.VMEM((2, FF, DIM), BF16),
        pltpu.VMEM((4, 2 * TOK, DIM), BF16),
        pltpu.VMEM((2 * TOK, DIM), BF16),
        pltpu.VMEM((NE, ROWS, DIM), BF16),
        pltpu.VMEM((NE, ROWS, FF), BF16),
        pltpu.VMEM((2, ALLR, CH), BF16),
        pltpu.VMEM((ALLR, 2 * TOK), BF16),
        pltpu.VMEM((2, 3, 2 * TOK, ALLR), BF16),
        pltpu.VMEM((NCH, TOK, CH), F32),
        pltpu.VMEM((NCH, TOK, CH), F32),
        pltpu.VMEM((NCH, TOK, CH), F32),
        pltpu.VMEM((NCH, TOK, CH), F32),
        pltpu.VMEM((NCH, TOK, CH), F32),
        pltpu.VMEM((2 * NCH, TOK, CH), F32),
        pltpu.VMEM((2 * NCH, TOK, CH), F32),
        pltpu.VMEM((2, TOK, FF), BF16),
        pltpu.VMEM((2, TOK, FF), BF16),
        pltpu.VMEM((2, TOK, FF), BF16),
        pltpu.VMEM((2, TOK, DIM), BF16),
        pltpu.VMEM((4, 4, TOPK, TOK), jnp.int32),
        pltpu.VMEM((4, 2, TOPK, TOK), F32),
        pltpu.SemaphoreType.DMA((13,)),
        pltpu.SemaphoreType.DMA((NRING, 2)),
        pltpu.SemaphoreType.DMA((NE // W2G,)),
        pltpu.SemaphoreType.DMA((nsem,)),
        pltpu.SemaphoreType.DMA((nsem,)),
        pltpu.SemaphoreType.REGULAR,
    ]

    def layer_local(tokens_a, tokens_b, experts_a, experts_b, gates_a, gates_b, slots_a, slots_b, shared_w1, shared_w3, shared_w2, routed_w1, routed_w3, routed_w2):
        return pl.pallas_call(
            kernel,
            out_shape=(jax.ShapeDtypeStruct((TOK, DIM), BF16),) * 2,
            in_specs=[pl.BlockSpec(memory_space=pl.ANY)] * 14,
            out_specs=(pl.BlockSpec(memory_space=pl.ANY),) * 2,
            scratch_shapes=scratch,
            compiler_params=pltpu.CompilerParams(collective_id=0, has_side_effects=True, vmem_limit_bytes=67043328),
        )(tokens_a, tokens_b, experts_a.T, slots_a.T, experts_b.T, slots_b.T, gates_a.T, gates_b.T,
          shared_w1, shared_w3, shared_w2, routed_w1, routed_w3, routed_w2)

    return jax.shard_map(layer_local, mesh=mesh, in_specs=in_specs, out_specs=(tok_spec, tok_spec), check_vma=False)
```

```python
import functools

import jax
import jax.numpy as jnp
from jax import lax
from jax.experimental import pallas as pl
from jax.experimental.pallas import tpu as pltpu
from jax.sharding import PartitionSpec as P

MESH = pl.DeviceIdType.MESH
F32, BF16 = jnp.float32, jnp.bfloat16

TOK = 128
DIM = 1536
FF = 512
TOPK = 6
CAP = 24
NE = 16
SRC = 8
ROWS = SRC * CAP
SROWS = NE * CAP
KC = 512
NK = DIM // KC
CH = 512
NCH = DIM // CH
NS = 24
N1 = NK * NE
N2 = NCH * NE // 2
BF16_MAX = 3.3895313892515355e38


def dot(a, b):
    return jnp.dot(a, b, preferred_element_type=F32)


def kernel(tok_a, tok_b, e_a, s_a, e_b, s_b, g_a, g_b, sw1, sw3, sw2, rw1, rw3, rw2,
           out_a, out_b,
           ring, sw13, sw2v, tok, ytok, buf, pf, hid, pmat, g3,
           recvr, recvl, xr, hso, hyo, hsi, ost, mi, mg,
           loc_sem, ring_sem, snd, rcv):
    tp = lax.axis_index('tp')
    ep = lax.axis_index('ep')
    core = lax.rem(ep, 2)
    first = ep * NE
    dev_d = {'ep': ep + 1 - 2 * core}
    dev_x = {'ep': lax.rem(ep + 2, 4)}
    dev_y = {'tp': 1 - tp}
    toks, ids, gates = (tok_a, tok_b), (e_a, s_a, e_b, s_b), (g_a, g_b)
    outs = (out_a, out_b)

    def local(src, dst, sem):
        return pltpu.make_async_copy(src, dst, loc_sem.at[sem])

    def remote(src, dst, sem, dev):
        return pltpu.make_async_remote_copy(src_ref=src, dst_ref=dst, send_sem=snd.at[sem], recv_sem=rcv.at[sem],
                                            device_id=dev, device_id_type=MESH)

    def mult(i, k):
        return i * k if isinstance(i, int) else pl.multiple_of(i * k, k)

    def part(i, k):
        return pl.ds(mult(i, k), k)

    own_meta = [local(ids[i], mi.at[0, i], i) for i in range(4)] + [local(gates[m], mg.at[0, m], 4 + m) for m in range(2)]
    own_tok = [local(toks[m], tok.at[2 * m, pl.ds(0, TOK)], 6 + m) for m in range(2)]
    shared = [local(sw1, sw13.at[0], 8), local(sw3, sw13.at[1], 9), local(sw2, sw2v.at[0], 10)]

    def put(m, c):
        cols = part(c, CH)
        return local(ost.at[m, :, cols], outs[m].at[:, cols], 11 + m * NCH + c)

    def first_item(n, slot):
        e, rows = n % NE, part(n // NE, KC)
        return (pltpu.make_async_copy(rw1.at[e, rows], ring.at[slot, pl.ds(0, KC)], ring_sem.at[slot, 0]),
                pltpu.make_async_copy(rw3.at[e, rows], ring.at[slot, pl.ds(KC, KC)], ring_sem.at[slot, 1]))

    def second_item(n, slot):
        g, cols = n % (NE // 2), part(n // (NE // 2), CH)
        return (pltpu.make_async_copy(rw2.at[2 * g, :, cols], ring.at[slot, pl.ds(0, FF)], ring_sem.at[slot, 0]),
                pltpu.make_async_copy(rw2.at[2 * g + 1, :, cols], ring.at[slot, pl.ds(FF, FF)], ring_sem.at[slot, 1]))

    def refill(n):
        slot = n % NS

        @pl.when(n < N1)
        def _():
            for c in first_item(n, slot):
                c.start()

        @pl.when((n >= N1) & (n < N1 + N2))
        def _():
            for c in second_item(n - N1, slot):
                c.start()

    d_meta = [remote(ids[i], mi.at[1, i], i, dev_d) for i in range(4)]
    d_meta += [remote(gates[m], mg.at[1, m], 4 + m, dev_d) for m in range(2)]
    x_meta = [remote(ids[i], mi.at[2, i], 6 + i, dev_x) for i in range(4)]
    x_meta += [remote(gates[m], mg.at[2, m], 10 + m, dev_x) for m in range(2)]
    f_meta = [remote(mi.at[2], mi.at[3], 12, dev_d), remote(mg.at[2], mg.at[3], 13, dev_d)]
    d_tok = [remote(toks[m], tok.at[2 * m, pl.ds(TOK, TOK)], 14 + m, dev_d) for m in range(2)]
    y_tok = [remote(toks[m], ytok.at[pl.ds(m * TOK, TOK)], 16 + m, dev_y) for m in range(2)]
    half = part(core, FF // 2)
    y_w2 = remote(sw2.at[half], sw2v.at[1, half], 18, dev_y)
    f_w2 = remote(sw2v.at[1, half], sw2v.at[1, half], 19, dev_d)
    y_hid = remote(hyo, hsi, 20, dev_y)
    x_tok, f_tok = [], []
    for k in range(NK):
        cols = part(k, KC)
        x_tok.append([remote(toks[m].at[:, cols], tok.at[2 * m + 1, pl.ds(0, TOK), cols], 21 + 2 * k + m, dev_x)
                      for m in range(2)])
        f_tok.append([remote(tok.at[2 * m + 1, pl.ds(0, TOK), cols], tok.at[2 * m + 1, pl.ds(TOK, TOK), cols],
                             21 + 2 * NK + 2 * k + m, dev_d) for m in range(2)])
    base_sem = 21 + 4 * NK

    def send_r(i):
        return part(i, TOK)

    def send_l(i):
        return part(2 * NCH + i, TOK)

    def send_x(i):
        return part(4 * NCH + i, TOK)

    def kept(i):
        return part(6 * NCH + i, TOK)

    def d_rem(i):
        return remote(pf.at[send_r(i)], recvr.at[i], base_sem + i, dev_d)

    def d_loc(i):
        return remote(pf.at[send_l(i)], recvl.at[i], base_sem + 2 * NCH + i, dev_d)

    def x_part(i):
        return remote(pf.at[send_x(i)], xr.at[i], base_sem + 4 * NCH + i, dev_x)

    def swiglu(rows, w1, w3):
        p1 = dot(rows, w1)
        p3 = dot(rows, w3)
        return (jax.nn.silu(p1) * p3).astype(BF16)

    def build(src):
        def block(i, _):
            m, b = i // (SROWS // 128), i % (SROWS // 128)
            at = part(b, 128)
            slot = mi[src, 2 * m + 1]
            el = mi[src, 2 * m] - first
            ok = (slot >= 0) & (el >= 0) & (el < NE)
            rid = jnp.where(ok, el * CAP + slot, -1) - b * 128
            g = mg[src, m]
            row = lax.broadcasted_iota(jnp.int32, (128, TOK), 0)
            hit = jnp.zeros((128, TOK), F32)
            gt = jnp.zeros((128, TOK), F32)
            for j in range(TOPK):
                same = row == rid[j:j + 1, :]
                hit = jnp.where(same, 1.0, hit)
                gt = jnp.where(same, g[j:j + 1, :], gt)
            pmat[4 * m + src, at, :] = hit.astype(BF16)
            gg = gt.T
            hi = jnp.minimum(gg, BF16_MAX).astype(BF16)
            r1 = gg - hi.astype(F32)
            mid = r1.astype(BF16)
            lo = (r1 - mid.astype(F32)).astype(BF16)
            for k, v in enumerate((hi, mid, lo)):
                g3[4 * m + src, k * TOK:(k + 1) * TOK, at] = v
            return 0
        lax.fori_loop(0, 2 * SROWS // 128, block, 0)

    def dispatch(k, pair):
        def group(i, _):
            m, cols = i // (KC // 256), pl.ds(pl.multiple_of(k * KC + (i % (KC // 256)) * 256, 256), 256)
            to = part(i % (KC // 256), 256)
            s = 4 * m + 2 * pair
            r0 = dot(pmat[s], tok[2 * m + pair, pl.ds(0, TOK), cols])
            r1 = dot(pmat[s + 1], tok[2 * m + pair, pl.ds(TOK, TOK), cols])
            for e in range(NE):
                both = jnp.concatenate([r0[e * CAP:(e + 1) * CAP], r1[e * CAP:(e + 1) * CAP]], axis=0)
                buf[pl.ds(pl.multiple_of(e * ROWS + s * CAP, 2 * CAP), 2 * CAP), to] = both.astype(BF16)
            return 0
        lax.fori_loop(0, 2 * (KC // 256), group, 0)

    def stage1(k):
        def step(i, _):
            for u in range(2):
                n = k * NE + 2 * i + u
                for c in first_item(n, n % NS):
                    c.wait()
            for u in range(2):
                e = 2 * i + u
                n = k * NE + e
                slot = n % NS
                rows = buf[part(e, ROWS), :]
                p1 = dot(rows, ring[slot, :KC])
                p3 = dot(rows, ring[slot, KC:])
                at1, at3 = part(2 * e, ROWS), part(2 * e + 1, ROWS)
                if k:
                    p1 = p1 + pf[at1, :]
                    p3 = p3 + pf[at3, :]
                if k < NK - 1:
                    pf[at1, :] = p1
                    pf[at3, :] = p3
                else:
                    hid[e] = (jax.nn.silu(p1) * p3).astype(BF16)
            for u in range(2):
                refill(k * NE + 2 * i + u + NS)
            return 0
        lax.fori_loop(0, NE // 2, step, 0)

    def combine(s):
        q = dot(g3[s], buf[part(s, SROWS), :])
        return q[:TOK] + q[TOK:2 * TOK] + q[2 * TOK:]

    def stage2(c):
        def step(g, _):
            n = c * (NE // 2) + g
            slot = (N1 + n) % NS
            for d in second_item(n, slot):
                d.wait()
            r0 = dot(hid[2 * g], ring[slot, :FF])
            r1 = dot(hid[2 * g + 1], ring[slot, FF:])
            for s in range(SRC):
                both = jnp.concatenate([r0[s * CAP:(s + 1) * CAP], r1[s * CAP:(s + 1) * CAP]], axis=0)
                buf[pl.ds(pl.multiple_of(s * SROWS + g * 2 * CAP, 2 * CAP), 2 * CAP), :] = both.astype(BF16)
            refill(N1 + n + NS)
            return 0
        lax.fori_loop(0, NE // 2, step, 0)

        def to_die(m, _):
            pf[send_r(m * NCH + c), :] = combine(4 * m + 3)
            d_rem(m * NCH + c).start()
            return 0
        lax.fori_loop(0, 2, to_die, 0)

        def mine(m, _):
            pf[send_x(m * NCH + c), :] = combine(4 * m + 2)
            return 0
        lax.fori_loop(0, 2, mine, 0)

        def to_x(m, _):
            i = m * NCH + c
            d_rem(i).wait_recv()
            pf[send_x(i), :] = pf[send_x(i), :] + recvr[i]
            x_part(i).start()
            return 0
        lax.fori_loop(0, 2, to_x, 0)

        def home(m, _):
            i = m * NCH + c
            pf[send_l(i), :] = combine(4 * m + 1)
            d_loc(i).start()
            pf[kept(i), :] = combine(4 * m)
            return 0
        lax.fori_loop(0, 2, home, 0)

    for c in own_meta + own_tok:
        c.start()
    barrier = pltpu.get_barrier_semaphore()
    for dev in (dev_d, dev_x, dev_y):
        pl.semaphore_signal(barrier, inc=1, device_id=dev, device_id_type=MESH)
    pl.semaphore_wait(barrier, 3)
    for c in x_meta + d_meta + x_tok[0] + d_tok + x_tok[1] + x_tok[2] + y_tok + [y_w2]:
        c.start()
    for c in own_meta + own_tok:
        c.wait()
    for c in shared[:2]:
        c.start()

    def fill(n, _):
        for c in first_item(n, n):
            c.start()
        return 0
    lax.fori_loop(0, NS, fill, 0)
    shared[2].start()

    build(0)
    for c in d_meta + x_meta:
        c.wait_recv()
    for c in f_meta:
        c.start()
    build(1)
    build(2)
    for c in f_meta + d_tok:
        c.wait_recv()
    build(3)
    for c in shared[:2]:
        c.wait()
    for m in range(2):
        hso[m] = swiglu(tok[2 * m, :TOK], sw13[0], sw13[1])

    for k in range(NK):
        for c in x_tok[k]:
            c.wait_recv()
        for c in f_tok[k]:
            c.start()
        dispatch(k, 0)
        for c in f_tok[k]:
            c.wait_recv()
        dispatch(k, 1)
        stage1(k)

    stage2(0)
    for c in y_tok:
        c.wait_recv()
    for m in range(2):
        hyo[m] = swiglu(ytok[m * TOK:(m + 1) * TOK], sw13[0], sw13[1])
    y_hid.start()
    for c in range(1, NCH):
        stage2(c)
    y_w2.wait_recv()
    f_w2.start()
    shared[2].wait()
    f_w2.wait_recv()
    y_hid.wait_recv()

    for m in range(2):
        def base(c, _, m=m):
            cols, i = part(c, CH), m * NCH + c
            d_loc(i).wait_recv()
            s = dot(hso[m], sw2v[0, :, cols]) + dot(hsi[m], sw2v[1, :, cols])
            pf[kept(i), :] = pf[kept(i), :] + recvl[i] + s + tok[2 * m, pl.ds(0, TOK), cols].astype(F32)
            return 0
        lax.fori_loop(0, NCH, base, 0)

    for c in range(NCH):
        for m in range(2):
            i = m * NCH + c
            x_part(i).wait_recv()
            ost[m, :, c * CH:(c + 1) * CH] = (pf[kept(i), :] + xr[i]).astype(BF16)
            put(m, c).start()

    for c in x_meta + d_meta + f_meta + d_tok + y_tok + [y_w2, f_w2, y_hid] + sum(x_tok, []) + sum(f_tok, []):
        c.wait_send()
    for i in range(2 * NCH):
        d_rem(i).wait_send()
        d_loc(i).wait_send()
        x_part(i).wait_send()
    for m in range(2):
        for c in range(NCH):
            put(m, c).wait()


def solution(mesh):
    tok_spec = P(('data', 'ep', 'tp'), None)
    in_specs = (tok_spec,) * 8 + (P(None, 'tp'), P(None, 'tp'), P('tp', None), P('ep', None, None), P('ep', None, None), P('ep', None, None))
    nsem = 21 + 4 * NK + 6 * NCH
    scratch = [
        pltpu.VMEM((NS, 2 * KC, FF), BF16),
        pltpu.VMEM((2, DIM, FF), BF16),
        pltpu.VMEM((2, FF, DIM), BF16),
        pltpu.VMEM((4, 2 * TOK, DIM), BF16),
        pltpu.VMEM((2 * TOK, DIM), BF16),
        pltpu.VMEM((NE * ROWS, KC), BF16),
        pltpu.VMEM((2 * NE * ROWS, FF), F32),
        pltpu.VMEM((NE, ROWS, FF), BF16),
        pltpu.VMEM((SRC, SROWS, TOK), BF16),
        pltpu.VMEM((SRC, 3 * TOK, SROWS), BF16),
        pltpu.VMEM((2 * NCH, TOK, CH), F32),
        pltpu.VMEM((2 * NCH, TOK, CH), F32),
        pltpu.VMEM((2 * NCH, TOK, CH), F32),
        pltpu.VMEM((2, TOK, FF), BF16),
        pltpu.VMEM((2, TOK, FF), BF16),
        pltpu.VMEM((2, TOK, FF), BF16),
        pltpu.VMEM((2, TOK, DIM), BF16),
        pltpu.VMEM((4, 4, TOPK, TOK), jnp.int32),
        pltpu.VMEM((4, 2, TOPK, TOK), F32),
        pltpu.SemaphoreType.DMA((11 + 2 * NCH,)),
        pltpu.SemaphoreType.DMA((NS, 2)),
        pltpu.SemaphoreType.DMA((nsem,)),
        pltpu.SemaphoreType.DMA((nsem,)),
    ]

    def layer_local(tokens_a, tokens_b, experts_a, experts_b, gates_a, gates_b, slots_a, slots_b, shared_w1, shared_w3, shared_w2, routed_w1, routed_w3, routed_w2):
        return pl.pallas_call(
            kernel,
            out_shape=(jax.ShapeDtypeStruct((TOK, DIM), BF16),) * 2,
            in_specs=[pl.BlockSpec(memory_space=pl.ANY)] * 14,
            out_specs=(pl.BlockSpec(memory_space=pl.ANY),) * 2,
            scratch_shapes=scratch,
            compiler_params=pltpu.CompilerParams(collective_id=0, has_side_effects=True, vmem_limit_bytes=67043328),
        )(tokens_a, tokens_b, experts_a.T, slots_a.T, experts_b.T, slots_b.T, gates_a.T, gates_b.T,
          shared_w1, shared_w3, shared_w2, routed_w1, routed_w3, routed_w2)

    return jax.shard_map(layer_local, mesh=mesh, in_specs=in_specs, out_specs=(tok_spec, tok_spec), check_vma=False)
```

```python
import functools

import jax
import jax.numpy as jnp
from jax import lax
from jax.experimental import pallas as pl
from jax.experimental.pallas import tpu as pltpu
from jax.sharding import PartitionSpec as P

MESH = pl.DeviceIdType.MESH
F32, BF16 = jnp.float32, jnp.bfloat16

TOK = 128
DIM = 1536
FF = 512
TOPK = 6
CAP = 24
NE = 16
SRC = 8
ROWS = SRC * CAP
SROWS = NE * CAP
KC = 512
NK = DIM // KC
CHS = (256, 512, 512, 256)
NCH = len(CHS)
COL = [sum(CHS[:c]) for c in range(NCH)]
NS = 24
N1 = NK * NE
ITEM2 = [N1 + COL[c] // 64 for c in range(NCH)]
NITEM = N1 + DIM // 64
BF16_MAX = 3.3895313892515355e38


def dot(a, b):
    return jnp.dot(a, b, preferred_element_type=F32)


def kernel(tok_a, tok_b, e_a, s_a, e_b, s_b, g_a, g_b, sw1, sw3, sw2, rw1, rw3, rw2,
           out_ab,
           ring, sw13, sw2v, tok, ytok, buf, pf, hid, pmat, g3,
           recvr, recvl, xr, hso, hyo, hsi, ost, mi, mg,
           loc_sem, ring_sem, snd, rcv):
    tp = lax.axis_index('tp')
    ep = lax.axis_index('ep')
    core = lax.rem(ep, 2)
    first = ep * NE
    dev_d = {'ep': ep + 1 - 2 * core}
    dev_x = {'ep': lax.rem(ep + 2, 4)}
    dev_y = {'tp': 1 - tp}
    toks, ids, gates = (tok_a, tok_b), (e_a, s_a, e_b, s_b), (g_a, g_b)

    def local(src, dst, sem):
        return pltpu.make_async_copy(src, dst, loc_sem.at[sem])

    def remote(src, dst, sem, dev):
        return pltpu.make_async_remote_copy(src_ref=src, dst_ref=dst, send_sem=snd.at[sem], recv_sem=rcv.at[sem],
                                            device_id=dev, device_id_type=MESH)

    def mult(i, k):
        return i * k if isinstance(i, int) else pl.multiple_of(i * k, k)

    def part(i, k):
        return pl.ds(mult(i, k), k)

    own_meta = [local(ids[i], mi.at[0, i], i) for i in range(4)] + [local(gates[m], mg.at[0, m], 4 + m) for m in range(2)]
    own_tok = [local(toks[m], tok.at[0, m], 6 + m) for m in range(2)]
    shared = [local(sw1, sw13.at[0], 8), local(sw3, sw13.at[1], 9), local(sw2, sw2v.at[0], 10)]

    def out_cols(c):
        return pl.ds(COL[c], CHS[c])

    def put(m, c):
        return local(ost.at[m, :, out_cols(c)], out_ab.at[m, :, out_cols(c)], 11 + m * NCH + c)

    def first_item(n, slot):
        e, rows = n % NE, part(n // NE, KC)
        return (pltpu.make_async_copy(rw1.at[e, rows], ring.at[slot, pl.ds(0, KC)], ring_sem.at[slot, 0]),
                pltpu.make_async_copy(rw3.at[e, rows], ring.at[slot, pl.ds(KC, KC)], ring_sem.at[slot, 1]))

    def second_item(c, q, slot):
        w = CHS[c]
        per_row = FF // w
        res = []
        for i in range(2 * per_row):
            to = ring.at[slot, pl.ds((i // per_row) * FF, FF), pl.ds((i % per_row) * w, w)]
            res.append(pltpu.make_async_copy(rw2.at[2 * per_row * q + i, :, out_cols(c)], to, ring_sem.at[slot, i]))
        return res

    segments = [(0, N1, lambda n, slot: first_item(n, slot))]
    for c in range(NCH):
        stop = ITEM2[c + 1] if c + 1 < NCH else NITEM
        segments.append((ITEM2[c], stop, lambda n, slot, c=c: second_item(c, n - ITEM2[c], slot)))

    def refill(n, low, high):
        for a, b, copies in segments:
            if a >= high or b <= low:
                continue

            def go(copies=copies):
                for c in copies(n, n % NS):
                    c.start()
            if a <= low and high <= b:
                go()
            else:
                pl.when((n >= a) & (n < b))(go)

    d_meta = [remote(ids[i], mi.at[1, i], i, dev_d) for i in range(4)]
    d_meta += [remote(gates[m], mg.at[1, m], 4 + m, dev_d) for m in range(2)]
    x_meta = [remote(ids[i], mi.at[2, i], 6 + i, dev_x) for i in range(4)]
    x_meta += [remote(gates[m], mg.at[2, m], 10 + m, dev_x) for m in range(2)]
    f_meta = [remote(mi.at[2], mi.at[3], 12, dev_d), remote(mg.at[2], mg.at[3], 13, dev_d)]
    d_tok = [remote(toks[m], tok.at[1, m], 14 + m, dev_d) for m in range(2)]
    y_tok = [remote(toks[m], ytok.at[pl.ds(m * TOK, TOK)], 16 + m, dev_y) for m in range(2)]
    half = part(core, FF // 2)
    y_w2 = remote(sw2.at[half], sw2v.at[1, half], 18, dev_y)
    f_w2 = remote(sw2v.at[1, half], sw2v.at[1, half], 19, dev_d)
    y_hid = remote(hyo, hsi, 20, dev_y)
    x_tok, f_tok = [], []
    for k in range(NK):
        cols = part(k, KC)
        x_tok.append([remote(toks[m].at[:, cols], tok.at[2, m, :, cols], 21 + 2 * k + m, dev_x) for m in range(2)])
        f_tok.append([remote(tok.at[2, m, :, cols], tok.at[3, m, :, cols], 21 + 2 * NK + 2 * k + m, dev_d)
                      for m in range(2)])
    base_sem = 21 + 4 * NK

    def block(kind, m, c):
        return pf.at[pl.ds((kind * 2 * NCH + 2 * c + m) * TOK, TOK), pl.ds(0, CHS[c])]

    def send_r(m, c):
        return block(0, m, c)

    def send_l(m, c):
        return block(1, m, c)

    def send_x(m, c):
        return block(2, m, c)

    def kept(m, c):
        return block(3, m, c)

    def d_rem(m, c):
        return remote(send_r(m, c), recvr.at[m, :, out_cols(c)], base_sem + 2 * c + m, dev_d)

    def d_loc(m, c):
        return remote(send_l(m, c), recvl.at[m, :, out_cols(c)], base_sem + 2 * NCH + 2 * c + m, dev_d)

    def x_part(m, c):
        return remote(send_x(m, c), xr.at[m, :, out_cols(c)], base_sem + 4 * NCH + 2 * c + m, dev_x)

    def swiglu(rows, w1, w3):
        p1 = dot(rows, w1)
        p3 = dot(rows, w3)
        return (jax.nn.silu(p1) * p3).astype(BF16)

    def build(src):
        def rows_of(i, _):
            m, b = i // (SROWS // 128), i % (SROWS // 128)
            at = part(b, 128)
            slot = mi[src, 2 * m + 1]
            el = mi[src, 2 * m] - first
            ok = (slot >= 0) & (el >= 0) & (el < NE)
            rid = jnp.where(ok, el * CAP + slot, -1) - b * 128
            g = mg[src, m]
            row = lax.broadcasted_iota(jnp.int32, (128, TOK), 0)
            hit = jnp.zeros((128, TOK), F32)
            gt = jnp.zeros((128, TOK), F32)
            for j in range(TOPK):
                same = row == rid[j:j + 1, :]
                hit = jnp.where(same, 1.0, hit)
                gt = jnp.where(same, g[j:j + 1, :], gt)
            pmat[2 * src + m, at, :] = hit.astype(BF16)
            gg = gt.T
            hi = jnp.minimum(gg, BF16_MAX).astype(BF16)
            r1 = gg - hi.astype(F32)
            mid = r1.astype(BF16)
            lo = (r1 - mid.astype(F32)).astype(BF16)
            for k, v in enumerate((hi, mid, lo)):
                g3[2 * src + m, k * TOK:(k + 1) * TOK, at] = v
            return 0
        lax.fori_loop(0, 2 * SROWS // 128, rows_of, 0)

    def dispatch(k, src):
        cols = part(k, KC)
        r0 = dot(pmat[2 * src], tok[src, 0, :, cols])
        r1 = dot(pmat[2 * src + 1], tok[src, 1, :, cols])
        for e in range(NE):
            both = jnp.concatenate([r0[e * CAP:(e + 1) * CAP], r1[e * CAP:(e + 1) * CAP]], axis=0)
            at = e * ROWS + src * 2 * CAP
            buf[at:at + 2 * CAP, :] = both.astype(BF16)

    def stage1(k):
        per = 4

        def step(i, _):
            for u in range(per):
                n = k * NE + per * i + u
                for c in first_item(n, n % NS):
                    c.wait()
            for u in range(per):
                e = per * i + u
                slot = (k * NE + e) % NS
                rows = buf[part(e, ROWS), :]
                p1 = dot(rows, ring[slot, :KC])
                p3 = dot(rows, ring[slot, KC:])
                at1, at3 = part(2 * e, ROWS), part(2 * e + 1, ROWS)
                if k:
                    p1 = p1 + pf[at1, :]
                    p3 = p3 + pf[at3, :]
                if k < NK - 1:
                    pf[at1, :] = p1
                    pf[at3, :] = p3
                else:
                    hid[e] = (jax.nn.silu(p1) * p3).astype(BF16)
            for u in range(per):
                refill(k * NE + per * i + u + NS, k * NE + NS, (k + 1) * NE + NS)
            return 0
        lax.fori_loop(0, NE // per, step, 0)

    def combine(s, w):
        q = dot(g3[s], buf[s * SROWS:(s + 1) * SROWS, :w])
        return q[:TOK] + q[TOK:2 * TOK] + q[2 * TOK:]

    def stage2(c):
        w = CHS[c]
        per_row = FF // w
        items = 2 // per_row

        def step(q, _):
            r = []
            for i in range(items):
                for d in second_item(c, q * items + i, (ITEM2[c] + q * items + i) % NS):
                    d.wait()
            for i in range(4):
                slot = (ITEM2[c] + q * items + i // (4 // items)) % NS
                j = i % (4 // items)
                a, b = (j // per_row) * FF, (j % per_row) * w
                r.append(dot(hid[4 * q + i], ring[slot, a:a + FF, b:b + w]))
            for s in range(SRC):
                rows = jnp.concatenate([v[s * CAP:(s + 1) * CAP] for v in r], axis=0)
                buf[pl.ds(pl.multiple_of(s * SROWS + q * 4 * CAP, 4 * CAP), 4 * CAP), :w] = rows.astype(BF16)
            for i in range(items):
                low = ITEM2[c] + NS
                refill(ITEM2[c] + q * items + i + NS, low, low + 4 * items)
            return 0
        lax.fori_loop(0, 4, step, 0)

        for m in range(2):
            send_r(m, c)[...] = combine(6 + m, w)
            d_rem(m, c).start()
        for m in range(2):
            send_x(m, c)[...] = combine(4 + m, w)
        for m in range(2):
            send_l(m, c)[...] = combine(2 + m, w)
            d_loc(m, c).start()
        for m in range(2):
            d_rem(m, c).wait_recv()
            send_x(m, c)[...] = send_x(m, c)[...] + recvr[m, :, COL[c]:COL[c] + w]
            x_part(m, c).start()
        for m in range(2):
            kept(m, c)[...] = combine(m, w)

    for c in own_meta + own_tok:
        c.start()
    barrier = pltpu.get_barrier_semaphore()
    for dev in (dev_d, dev_x, dev_y):
        pl.semaphore_signal(barrier, inc=1, device_id=dev, device_id_type=MESH)
    pl.semaphore_wait(barrier, 3)
    for c in x_meta + d_meta + x_tok[0] + d_tok + x_tok[1] + x_tok[2] + y_tok + [y_w2]:
        c.start()
    for c in own_meta + own_tok:
        c.wait()
    for c in shared[:2]:
        c.start()

    def fill(n, _):
        for c in first_item(n, n):
            c.start()
        return 0
    lax.fori_loop(0, NS, fill, 0)
    shared[2].start()

    build(0)
    for c in d_meta + x_meta:
        c.wait_recv()
    for c in f_meta:
        c.start()
    build(1)
    build(2)
    for c in f_meta + d_tok:
        c.wait_recv()
    build(3)
    for c in shared[:2]:
        c.wait()
    for m in range(2):
        hso[m] = swiglu(tok[0, m], sw13[0], sw13[1])

    for k in range(NK):
        if k == 0:
            dispatch(k, 0)
            dispatch(k, 1)
        for c in x_tok[k]:
            c.wait_recv()
        for c in f_tok[k]:
            c.start()
        if k:
            dispatch(k, 0)
            dispatch(k, 1)
        dispatch(k, 2)
        for c in f_tok[k]:
            c.wait_recv()
        dispatch(k, 3)
        stage1(k)

    for c in range(NCH):
        stage2(c)
        if c == 1:
            for d in y_tok:
                d.wait_recv()
            for m in range(2):
                hyo[m] = swiglu(ytok[m * TOK:(m + 1) * TOK], sw13[0], sw13[1])
            y_hid.start()
    y_w2.wait_recv()
    f_w2.start()
    shared[2].wait()
    f_w2.wait_recv()
    y_hid.wait_recv()

    for c in range(NCH):
        at = slice(COL[c], COL[c] + CHS[c])
        for m in range(2):
            d_loc(m, c).wait_recv()
            s = dot(hso[m], sw2v[0, :, at]) + dot(hsi[m], sw2v[1, :, at])
            kept(m, c)[...] = kept(m, c)[...] + recvl[m, :, at] + s + tok[0, m, :, at].astype(F32)
    for c in range(NCH):
        at = slice(COL[c], COL[c] + CHS[c])
        for m in range(2):
            x_part(m, c).wait_recv()
            ost[m, :, at] = (kept(m, c)[...] + xr[m, :, at]).astype(BF16)
            put(m, c).start()

    for c in x_meta + d_meta + f_meta + d_tok + y_tok + [y_w2, f_w2, y_hid] + sum(x_tok, []) + sum(f_tok, []):
        c.wait_send()
    for c in range(NCH):
        for m in range(2):
            d_rem(m, c).wait_send()
            d_loc(m, c).wait_send()
            x_part(m, c).wait_send()
            put(m, c).wait()


def solution(mesh):
    tok_spec = P(('data', 'ep', 'tp'), None)
    in_specs = (tok_spec,) * 8 + (P(None, 'tp'), P(None, 'tp'), P('tp', None), P('ep', None, None), P('ep', None, None), P('ep', None, None))
    nsem = 21 + 4 * NK + 6 * NCH
    scratch = [
        pltpu.VMEM((NS, 2 * KC, FF), BF16),
        pltpu.VMEM((2, DIM, FF), BF16),
        pltpu.VMEM((2, FF, DIM), BF16),
        pltpu.VMEM((4, 2, TOK, DIM), BF16),
        pltpu.VMEM((2 * TOK, DIM), BF16),
        pltpu.VMEM((NE * ROWS, KC), BF16),
        pltpu.VMEM((2 * NE * ROWS, FF), F32),
        pltpu.VMEM((NE, ROWS, FF), BF16),
        pltpu.VMEM((SRC, SROWS, TOK), BF16),
        pltpu.VMEM((SRC, 3 * TOK, SROWS), BF16),
        pltpu.VMEM((2, TOK, DIM), F32),
        pltpu.VMEM((2, TOK, DIM), F32),
        pltpu.VMEM((2, TOK, DIM), F32),
        pltpu.VMEM((2, TOK, FF), BF16),
        pltpu.VMEM((2, TOK, FF), BF16),
        pltpu.VMEM((2, TOK, FF), BF16),
        pltpu.VMEM((2, TOK, DIM), BF16),
        pltpu.VMEM((4, 4, TOPK, TOK), jnp.int32),
        pltpu.VMEM((4, 2, TOPK, TOK), F32),
        pltpu.SemaphoreType.DMA((11 + 2 * NCH,)),
        pltpu.SemaphoreType.DMA((NS, 4)),
        pltpu.SemaphoreType.DMA((nsem,)),
        pltpu.SemaphoreType.DMA((nsem,)),
    ]

    def layer_local(tokens_a, tokens_b, experts_a, experts_b, gates_a, gates_b, slots_a, slots_b, shared_w1, shared_w3, shared_w2, routed_w1, routed_w3, routed_w2):
        both = pl.pallas_call(
            kernel,
            out_shape=jax.ShapeDtypeStruct((2, TOK, DIM), BF16),
            in_specs=[pl.BlockSpec(memory_space=pl.ANY)] * 14,
            out_specs=pl.BlockSpec(memory_space=pl.ANY),
            scratch_shapes=scratch,
            compiler_params=pltpu.CompilerParams(collective_id=0, has_side_effects=True, vmem_limit_bytes=67043328),
        )(tokens_a, tokens_b, experts_a.T, slots_a.T, experts_b.T, slots_b.T, gates_a.T, gates_b.T,
          shared_w1, shared_w3, shared_w2, routed_w1, routed_w3, routed_w2)
        return both[0], both[1]

    return jax.shard_map(layer_local, mesh=mesh, in_specs=in_specs, out_specs=(tok_spec, tok_spec), check_vma=False)
```

```python
import functools

import jax
import jax.numpy as jnp
from jax import lax
from jax.experimental import pallas as pl
from jax.experimental.pallas import tpu as pltpu
from jax.sharding import PartitionSpec as P

MESH = pl.DeviceIdType.MESH
F32, BF16 = jnp.float32, jnp.bfloat16

TOK = 128
DIM = 1536
FF = 512
TOPK = 6
CAP = 24
NE = 16
SRC = 4
ROWS = SRC * CAP
SROWS = NE * CAP
KC = 512
NK = DIM // KC
CH = 256
NCH = DIM // CH
EARLY = 3
NS = 24
N1 = NK * NE
BF16_MAX = 3.3895313892515355e38


def dot(a, b):
    return jnp.dot(a, b, preferred_element_type=F32)


def kernel(tok_a, tok_b, e_a, s_a, e_b, s_b, g_a, g_b, sw1, sw3, sw2, rw1, rw3, rw2,
           out_ab, out_kept, out_x,
           ring, sw13, sw2v, tok, ytok, buf, pf, hid, pmat, g3,
           recvr, recvl, xr, hso, hyo, hsi, ost, mi, mg,
           loc_sem, ring_sem, snd, rcv):
    tp = lax.axis_index('tp')
    ep = lax.axis_index('ep')
    core = lax.rem(ep, 2)
    first = ep * NE
    dev_d = {'ep': ep + 1 - 2 * core}
    dev_x = {'ep': lax.rem(ep + 2, 4)}
    dev_y = {'tp': 1 - tp}
    toks, ids, gates = (tok_a, tok_b), (e_a, s_a, e_b, s_b), (g_a, g_b)

    def local(src, dst, sem):
        return pltpu.make_async_copy(src, dst, loc_sem.at[sem])

    def remote(src, dst, sem, dev):
        return pltpu.make_async_remote_copy(src_ref=src, dst_ref=dst, send_sem=snd.at[sem], recv_sem=rcv.at[sem],
                                            device_id=dev, device_id_type=MESH)

    def mult(i, k):
        return i * k if isinstance(i, int) else pl.multiple_of(i * k, k)

    def part(i, k):
        return pl.ds(mult(i, k), k)

    own = [local(ids[i], mi.at[0, i], 0) for i in range(4)] + [local(gates[m], mg.at[0, m], 1) for m in range(2)]
    own += [local(toks[m], tok.at[0, m], 2) for m in range(2)]
    own_all = [local(mi.at[1], mi.at[0], 0), local(mg.at[1], mg.at[0], 1), local(tok.at[1], tok.at[0], 2)]
    shared = [local(sw1, sw13.at[0], 3), local(sw3, sw13.at[1], 4), local(sw2, sw2v.at[0], 5)]

    def out_cols(c):
        return part(c, CH)

    def put(m, c):
        if c == NCH - 1:
            return local(kept(m, c), out_kept.at[m], 6)
        return local(ost.at[m, :, out_cols(c)], out_ab.at[m, :, out_cols(c)], 7)

    def first_item(n, slot):
        e, rows = n % NE, part(n // NE, KC)
        return (pltpu.make_async_copy(rw1.at[e, rows], ring.at[slot, pl.ds(0, KC)], ring_sem.at[slot]),
                pltpu.make_async_copy(rw3.at[e, rows], ring.at[slot, pl.ds(KC, KC)], ring_sem.at[slot]))

    def second_item(c, q, slot):
        return [pltpu.make_async_copy(rw2.at[4 * q + i, :, out_cols(c)],
                                      ring.at[slot, pl.ds((i // 2) * FF, FF), pl.ds((i % 2) * CH, CH)],
                                      ring_sem.at[slot]) for i in range(4)]

    def load2(c, slot0):
        def go(q, _):
            for d in second_item(c, q, slot0 + q):
                d.start()
            return 0
        lax.fori_loop(0, NE // 4, go, 0)

    def wait_item(slot):
        pltpu.make_async_copy(rw1.at[0, pl.ds(0, 2 * KC)], ring.at[slot], ring_sem.at[slot]).wait()

    def refill(n, low, high):
        def one():
            for d in first_item(n, n % NS):
                d.start()

        def two():
            for d in second_item((n - N1) // 4, (n - N1) % 4, n % NS):
                d.start()
        if high <= N1:
            one()
        elif low >= N1:
            two()
        else:
            pl.when(n < N1)(one)
            pl.when(n >= N1)(two)

    def same(ref, sem, dev):
        return remote(ref, ref, sem, dev)

    d_meta = [remote(ids[i], mi.at[1, i], 0, dev_d) for i in range(4)] + [remote(gates[m], mg.at[1, m], 1, dev_d) for m in range(2)]
    d_meta_all = [same(mi.at[1], 0, dev_d), same(mg.at[1], 1, dev_d)]
    x_meta = [remote(ids[i], mi.at[2, i], 2, dev_x) for i in range(4)] + [remote(gates[m], mg.at[2, m], 3, dev_x) for m in range(2)]
    x_meta_all = [same(mi.at[2], 2, dev_x), same(mg.at[2], 3, dev_x)]
    f_meta = [remote(mi.at[2], mi.at[3], 4, dev_d), remote(mg.at[2], mg.at[3], 5, dev_d)]
    d_tok = [remote(toks[m], tok.at[1, m], 6, dev_d) for m in range(2)]
    d_tok_all = same(tok.at[1], 6, dev_d)
    y_tok = [remote(toks[m], ytok.at[pl.ds(m * TOK, TOK)], 7, dev_y) for m in range(2)]
    y_tok_all = same(ytok, 7, dev_y)
    half = part(core, FF // 2)
    y_w2 = remote(sw2.at[half], sw2v.at[1, half], 8, dev_y)
    f_w2 = remote(sw2v.at[1, half], sw2v.at[1, half], 9, dev_d)
    y_hid = remote(hyo, hsi, 10, dev_y)
    x_tok, f_tok = [], []
    for k in range(NK):
        cols = part(k, KC)
        x_tok.append([remote(toks[m].at[:, cols], tok.at[2, m, :, cols], 11 + 2 * k + m, dev_x) for m in range(2)])
        f_tok.append([remote(tok.at[2, m, :, cols], tok.at[3, m, :, cols], 11 + 2 * NK + 2 * k + m, dev_d) for m in range(2)])
    base_sem = 11 + 4 * NK
    loc_of = base_sem + NCH + EARLY

    def block(kind, m, c):
        return pf.at[m, pl.ds((kind * NCH + c) * TOK, TOK), pl.ds(0, CH)]

    def send_r(m, c):
        return block(0, m, c)

    def send_l(m, c):
        return block(1, m, c)

    def send_x(m, c):
        return block(2, m, c)

    def kept(m, c):
        return block(3, m, c)

    def d_rem(m, c):
        return remote(send_r(m, c), recvr.at[m, :, out_cols(c)], base_sem + (2 * c + m if c < EARLY else c + EARLY), dev_d)

    def d_rem_all(c, ms):
        if len(ms) == 1:
            return d_rem(ms[0], c)
        return same(recvr.at[:, :, out_cols(c)], base_sem + c + EARLY, dev_d)

    def d_loc(m, c):
        return remote(send_l(m, c), recvl.at[m, :, out_cols(c)], loc_of, dev_d)

    d_loc_all = same(recvl, loc_of, dev_d)

    def x_part(m, c):
        to = out_x.at[m] if c == NCH - 1 else xr.at[m, :, out_cols(c)]
        return remote(send_x(m, c), to, loc_of + 1 + max(c - (NCH - 3), 0), dev_x)

    x_part_all = [same(xr.at[:, :, pl.ds(0, (NCH - 2) * CH)], loc_of + 1, dev_x),
                  same(xr.at[:, :, out_cols(NCH - 2)], loc_of + 2, dev_x),
                  same(out_x, loc_of + 3, dev_x)]

    def swiglu(rows, w1, w3):
        p1 = dot(rows, w1)
        p3 = dot(rows, w3)
        return (jax.nn.silu(p1) * p3).astype(BF16)

    def build(src):
        def rows_of(i, _):
            m, b = i // (SROWS // 128), i % (SROWS // 128)
            at = part(b, 128)
            slot = mi[src, 2 * m + 1]
            el = mi[src, 2 * m] - first
            ok = (slot >= 0) & (el >= 0) & (el < NE)
            rid = jnp.where(ok, el * CAP + slot, -1) - b * 128
            g = mg[src, m]
            row = lax.broadcasted_iota(jnp.int32, (128, TOK), 0)
            hit = jnp.zeros((128, TOK), F32)
            gt = jnp.zeros((128, TOK), F32)
            for j in range(TOPK):
                same = row == rid[j:j + 1, :]
                hit = jnp.where(same, 1.0, hit)
                gt = jnp.where(same, g[j:j + 1, :], gt)
            pmat[SRC * m + src, at, :] = hit.astype(BF16)
            gg = gt.T
            hi = jnp.minimum(gg, BF16_MAX).astype(BF16)
            r1 = gg - hi.astype(F32)
            mid = r1.astype(BF16)
            lo = (r1 - mid.astype(F32)).astype(BF16)
            for k, v in enumerate((hi, mid, lo)):
                g3[SRC * m + src, k * TOK:(k + 1) * TOK, at] = v
            return 0
        lax.fori_loop(0, 2 * SROWS // 128, rows_of, 0)

    def dispatch(k, m, pair):
        cols = part(k, KC)
        r0 = dot(pmat[SRC * m + 2 * pair], tok[2 * pair, m, :, cols])
        r1 = dot(pmat[SRC * m + 2 * pair + 1], tok[2 * pair + 1, m, :, cols])
        for e in range(NE):
            both = jnp.concatenate([r0[e * CAP:(e + 1) * CAP], r1[e * CAP:(e + 1) * CAP]], axis=0)
            at = e * ROWS + pair * 2 * CAP
            buf[m, at:at + 2 * CAP, :] = both.astype(BF16)

    def load(ref, ms, at):
        return jnp.concatenate([ref[m, at, :] for m in ms], axis=0) if len(ms) > 1 else ref[ms[0], at, :]

    def stage1(k, ms, half=None, fresh=True, done=True):
        per = 8 if k < NK - 1 else 16

        def step(i, _):
            if fresh:
                for u in range(per):
                    wait_item((k * NE + per * i + u) % NS)
            for u in range(per):
                e = per * i + u
                slot = (k * NE + e) % NS
                rows = load(buf, ms, part(e, ROWS))
                p1 = dot(rows, ring[slot, :KC])
                p3 = dot(rows, ring[slot, KC:])
                at1, at3 = part(2 * e, ROWS), part(2 * e + 1, ROWS)
                if k:
                    p1 = p1 + load(pf, ms, at1)
                    p3 = p3 + load(pf, ms, at3)
                if k == NK - 1:
                    p1 = (jax.nn.silu(p1) * p3).astype(BF16)
                for j, m in enumerate(ms):
                    at = slice(j * ROWS, (j + 1) * ROWS)
                    if k < NK - 1:
                        pf[m, at1, :] = p1[at]
                        pf[m, at3, :] = p3[at]
                    else:
                        hid[m, e] = p1[at]
            if done:
                for u in range(per):
                    low = k * NE + NS if half is None else k * NE + NS + half * NE // 2
                    high = (k + 1) * NE + NS if half is None else low + NE // 2
                    refill(k * NE + per * i + u + NS, low, high)
            return 0
        if half is None:
            lax.fori_loop(0, NE // per, step, 0)
        else:
            lax.fori_loop(half * NE // per // 2, (half + 1) * NE // per // 2, step, 0)

    def combine(m, s):
        q = dot(g3[SRC * m + s], buf[m, s * SROWS:(s + 1) * SROWS, :CH])
        return q[:TOK] + q[TOK:2 * TOK] + q[2 * TOK:]

    def stage2(c, ms, slot0, fresh=True):
        loop = 2 if len(ms) > 1 else 4

        def step(q, _):
            r = []
            if fresh:
                for i in range(loop):
                    wait_item(slot0 + q * loop + i)
            for i in range(4 * loop):
                slot = slot0 + q * loop + i // 4
                a, b = (i % 4 // 2) * FF, (i % 2) * CH
                e = 4 * loop * q + i
                rows = jnp.concatenate([hid[m, e] for m in ms], axis=0) if len(ms) > 1 else hid[ms[0], e]
                r.append(dot(rows, ring[slot, a:a + FF, b:b + CH]))
            for j, m in enumerate(ms):
                for s in range(SRC):
                    low = j * ROWS + s * CAP
                    rows = jnp.concatenate([v[low:low + CAP] for v in r], axis=0)
                    k = 4 * CAP * loop
                    buf[m, pl.ds(pl.multiple_of(s * SROWS + q * k, 2 * CAP), k), :CH] = rows.astype(BF16)
            return 0
        lax.fori_loop(0, 4 // loop, step, 0)

        to_die = [combine(m, 3) for m in ms]
        to_x = [combine(m, 2) for m in ms]
        for m, v in zip(ms, to_die):
            send_r(m, c)[...] = v
            d_rem(m, c).start()
        for m, v in zip(ms, to_x):
            send_x(m, c)[...] = v
        to_die = [combine(m, 1) for m in ms]
        home = [combine(m, 0) for m in ms]
        for m, v in zip(ms, to_die):
            send_l(m, c)[...] = v
            d_loc(m, c).start()
        for m, v in zip(ms, home):
            kept(m, c)[...] = v

    def pass_on(c, ms):
        d_rem_all(c, ms).wait_recv()
        for m in ms:
            send_x(m, c)[...] = send_x(m, c)[...] + recvr[m, :, c * CH:(c + 1) * CH]
            x_part(m, c).start()

    def arrived(k, ms):
        for m in ms:
            x_tok[k][m].wait_recv()
            f_tok[k][m].start()

    barrier = pltpu.get_barrier_semaphore()
    for dev in (dev_d, dev_x, dev_y):
        pl.semaphore_signal(barrier, inc=1, device_id=dev, device_id_type=MESH)
    for c in own:
        c.start()

    def fill(n, _):
        for c in first_item(n, n):
            c.start()
        return 0
    lax.fori_loop(0, 8, fill, 0)
    pl.semaphore_wait(barrier, 3)
    for c in x_meta + d_meta + x_tok[0] + d_tok + x_tok[1] + x_tok[2] + y_tok + [y_w2]:
        c.start()
    lax.fori_loop(8, NS, fill, 0)
    for c in own_all:
        c.wait()

    build(0)
    for c in d_meta_all + x_meta_all:
        c.wait_recv()
    for c in f_meta:
        c.start()
    build(1)
    build(2)
    for c in f_meta + [d_tok_all]:
        c.wait_recv()
    build(3)

    both, a, b = (0, 1), (0,), (1,)
    for m in both:
        dispatch(0, m, 0)
    arrived(0, a)
    arrived(0, b)
    for m in both:
        f_tok[0][m].wait_recv()
        dispatch(0, m, 1)
    stage1(0, both)
    arrived(1, a)
    dispatch(1, 0, 0)
    arrived(1, b)
    dispatch(1, 1, 0)
    for m in both:
        f_tok[1][m].wait_recv()
        dispatch(1, m, 1)
    stage1(1, both, half=0)
    arrived(2, a)
    stage1(1, both, half=1)
    dispatch(2, 0, 0)
    f_tok[2][0].wait_recv()
    dispatch(2, 0, 1)
    stage1(2, a, done=False)
    arrived(2, b)

    stage2(0, a, 0)
    load2(2, 0)
    dispatch(2, 1, 0)
    pass_on(0, a)
    stage2(1, a, 4)
    f_tok[2][1].wait_recv()
    dispatch(2, 1, 1)
    pass_on(1, a)
    stage2(2, a, 0)
    for c in shared:
        c.start()
    pass_on(2, a)
    stage1(2, b, fresh=False, done=False)
    load2(0, 8)
    load2(3, 12)
    load2(4, 16)
    load2(5, 20)
    stage2(1, b, 4, fresh=False)
    pass_on(1, b)
    stage2(2, b, 0, fresh=False)
    pass_on(2, b)
    stage2(0, b, 8)
    pass_on(0, b)
    stage2(3, both, 12)
    pass_on(3, both)
    for c in shared:
        c.wait()
    y_tok_all.wait_recv()
    for m in both:
        hyo[m] = swiglu(ytok[m * TOK:(m + 1) * TOK], sw13[0], sw13[1])
    y_hid.start()
    stage2(4, both, 16)
    pass_on(4, both)
    stage2(5, both, 20)
    pass_on(5, both)
    for m in both:
        hso[m] = swiglu(tok[0, m], sw13[0], sw13[1])
    y_w2.wait_recv()
    f_w2.start()
    y_hid.wait_recv()
    d_loc_all.wait_recv()
    f_w2.wait_recv()

    for c in range(NCH - 1, -1, -1):
        at = slice(c * CH, (c + 1) * CH)
        for m in both:
            s = dot(hso[m], sw2v[0, :, at]) + dot(hsi[m], sw2v[1, :, at])
            kept(m, c)[...] = kept(m, c)[...] + recvl[m, :, at] + s + tok[0, m, :, at].astype(F32)
            if c == NCH - 1:
                put(m, c).start()
    for c in range(NCH - 1):
        at = slice(c * CH, (c + 1) * CH)
        if c == 0 or c == NCH - 2:
            x_part_all[min(c, 1)].wait_recv()
        for m in both:
            ost[m, :, at] = (kept(m, c)[...] + xr[m, :, at]).astype(BF16)
            put(m, c).start()

    for c in x_meta_all + d_meta_all + f_meta + [d_tok_all, y_tok_all, y_w2, f_w2, y_hid, d_loc_all]:
        c.wait_send()
    for c in sum(x_tok, []) + sum(f_tok, []) + x_part_all:
        c.wait_send()
    for c in range(NCH):
        for ms in ((both,) if c >= EARLY else (a, b)):
            d_rem_all(c, ms).wait_send()
    local(recvl.at[:, :, out_cols(NCH - 1)], out_kept, 6).wait()
    local(ost.at[:, :, pl.ds(0, DIM - CH)], out_ab.at[:, :, pl.ds(0, DIM - CH)], 7).wait()
    x_part_all[2].wait_recv()


def finish(most, kept, x, out_a, out_b, row, k_v, x_v, sem):
    ready = DIM - CH
    early = [pltpu.make_async_copy(most.at[m, :, pl.ds(0, ready)], row.at[m, :, pl.ds(0, ready)], sem.at[m]) for m in range(2)]
    late = [pltpu.make_async_copy(kept.at[m], k_v.at[m], sem.at[2 + m]) for m in range(2)]
    late += [pltpu.make_async_copy(x.at[m], x_v.at[m], sem.at[4 + m]) for m in range(2)]
    for c in late + early:
        c.start()
    for c in late:
        c.wait()
    for m in range(2):
        row[m, :, ready:] = (k_v[m] + x_v[m]).astype(BF16)
    back = []
    for m, out in enumerate((out_a, out_b)):
        early[m].wait()
        back.append(pltpu.make_async_copy(row.at[m], out, sem.at[6 + m]))
        back[m].start()
    for c in back:
        c.wait()


def solution(mesh):
    tok_spec = P(('data', 'ep', 'tp'), None)
    in_specs = (tok_spec,) * 8 + (P(None, 'tp'), P(None, 'tp'), P('tp', None), P('ep', None, None), P('ep', None, None), P('ep', None, None))
    nsem = 11 + 4 * NK + NCH + EARLY + 4
    scratch = [
        pltpu.VMEM((NS, 2 * KC, FF), BF16),
        pltpu.VMEM((2, DIM, FF), BF16),
        pltpu.VMEM((2, FF, DIM), BF16),
        pltpu.VMEM((4, 2, TOK, DIM), BF16),
        pltpu.VMEM((2 * TOK, DIM), BF16),
        pltpu.VMEM((2, NE * ROWS, KC), BF16),
        pltpu.VMEM((2, 2 * NE * ROWS, FF), F32),
        pltpu.VMEM((2, NE, ROWS, FF), BF16),
        pltpu.VMEM((2 * SRC, SROWS, TOK), BF16),
        pltpu.VMEM((2 * SRC, 3 * TOK, SROWS), BF16),
        pltpu.VMEM((2, TOK, DIM), F32),
        pltpu.VMEM((2, TOK, DIM), F32),
        pltpu.VMEM((2, TOK, DIM), F32),
        pltpu.VMEM((2, TOK, FF), BF16),
        pltpu.VMEM((2, TOK, FF), BF16),
        pltpu.VMEM((2, TOK, FF), BF16),
        pltpu.VMEM((2, TOK, DIM), BF16),
        pltpu.VMEM((4, 4, TOPK, TOK), jnp.int32),
        pltpu.VMEM((4, 2, TOPK, TOK), F32),
        pltpu.SemaphoreType.DMA((8,)),
        pltpu.SemaphoreType.DMA((NS,)),
        pltpu.SemaphoreType.DMA((nsem,)),
        pltpu.SemaphoreType.DMA((nsem,)),
    ]

    def layer_local(tokens_a, tokens_b, experts_a, experts_b, gates_a, gates_b, slots_a, slots_b, shared_w1, shared_w3, shared_w2, routed_w1, routed_w3, routed_w2):
        hbm = pl.BlockSpec(memory_space=pl.ANY)
        tail = jax.ShapeDtypeStruct((2, TOK, CH), F32)
        parts = pl.pallas_call(
            kernel,
            out_shape=(jax.ShapeDtypeStruct((2, TOK, DIM), BF16), tail, tail),
            in_specs=[hbm] * 14,
            out_specs=(hbm,) * 3,
            scratch_shapes=scratch,
            compiler_params=pltpu.CompilerParams(collective_id=0, has_side_effects=True, vmem_limit_bytes=67043328),
        )(tokens_a, tokens_b, experts_a.T, slots_a.T, experts_b.T, slots_b.T, gates_a.T, gates_b.T,
          shared_w1, shared_w3, shared_w2, routed_w1, routed_w3, routed_w2)
        return pl.pallas_call(
            finish,
            out_shape=(jax.ShapeDtypeStruct((TOK, DIM), BF16),) * 2,
            in_specs=[hbm] * 3,
            out_specs=(hbm,) * 2,
            scratch_shapes=[pltpu.VMEM((2, TOK, DIM), BF16), pltpu.VMEM((2, TOK, CH), F32),
                            pltpu.VMEM((2, TOK, CH), F32), pltpu.SemaphoreType.DMA((8,))],
        )(*parts)

    return jax.shard_map(layer_local, mesh=mesh, in_specs=in_specs, out_specs=(tok_spec, tok_spec), check_vma=False)
```

```python
import functools

import jax
import jax.numpy as jnp
from jax import lax
from jax.experimental import pallas as pl
from jax.experimental.pallas import tpu as pltpu
from jax.sharding import PartitionSpec as P

MESH = pl.DeviceIdType.MESH
F32, BF16 = jnp.float32, jnp.bfloat16

TOK = 128
DIM = 1536
FF = 512
TOPK = 6
CAP = 24
NE = 16
SRC = 4
ROWS = SRC * CAP
SROWS = NE * CAP
KC = 512
NK = DIM // KC
CH = 256
NCH = DIM // CH
NS = 24
N1 = NK * NE
N2 = NCH * NE // 4
NA = N1 + N2
NB = NA - NE
BF16_MAX = 3.3895313892515355e38


def dot(a, b):
    return jnp.dot(a, b, preferred_element_type=F32)


def kernel(tok_a, tok_b, e_a, s_a, e_b, s_b, g_a, g_b, sw1, sw3, sw2, rw1, rw3, rw2,
           out_ab, out_kept, out_x,
           ring, sw13, sw2v, tok, ytok, buf, pf, hid, pmat, g3,
           recvr, recvl, xr, hsi, mi, mg,
           loc_sem, ring_sem, snd, rcv):
    tp = lax.axis_index('tp')
    ep = lax.axis_index('ep')
    core = lax.rem(ep, 2)
    first = ep * NE
    dev_d = {'ep': ep + 1 - 2 * core}
    dev_x = {'ep': lax.rem(ep + 2, 4)}
    dev_y = {'tp': 1 - tp}
    toks, ids, gates = (tok_a, tok_b), (e_a, s_a, e_b, s_b), (g_a, g_b)

    def local(src, dst, sem):
        return pltpu.make_async_copy(src, dst, loc_sem.at[sem])

    def remote(src, dst, sem, dev):
        return pltpu.make_async_remote_copy(src_ref=src, dst_ref=dst, send_sem=snd.at[sem], recv_sem=rcv.at[sem],
                                            device_id=dev, device_id_type=MESH)

    def mult(i, k):
        return i * k if isinstance(i, int) else pl.multiple_of(i * k, k)

    def part(i, k):
        return pl.ds(mult(i, k), k)

    own = [local(ids[i], mi.at[0, i], 0) for i in range(4)] + [local(gates[m], mg.at[0, m], 1) for m in range(2)]
    own += [local(toks[m], tok.at[0, m], 2) for m in range(2)]
    own_all = [local(mi.at[1], mi.at[0], 0), local(mg.at[1], mg.at[0], 1), local(tok.at[1], tok.at[0], 2)]
    shared = [local(sw1, sw13.at[0], 3), local(sw3, sw13.at[1], 4), local(sw2, sw2v.at[0], 5)]

    def out_cols(c):
        return part(c, CH)

    def put(m, c):
        if c == NCH - 1:
            return local(kept(m, c), out_kept.at[m], 6)
        return local(ytok.at[part(m, TOK), out_cols(c)], out_ab.at[m, :, out_cols(c)], 7)

    def first_item(n, slot):
        e, rows = n % NE, part(n // NE, KC)
        return (pltpu.make_async_copy(rw1.at[e, rows], ring.at[slot, pl.ds(0, KC)], ring_sem.at[slot]),
                pltpu.make_async_copy(rw3.at[e, rows], ring.at[slot, pl.ds(KC, KC)], ring_sem.at[slot]))

    def second_item(c, q, slot):
        return [pltpu.make_async_copy(rw2.at[4 * q + i, :, out_cols(c)],
                                      ring.at[slot, pl.ds((i // 2) * FF, FF), pl.ds((i % 2) * CH, CH)],
                                      ring_sem.at[slot]) for i in range(4)]

    def wait_item(slot):
        pltpu.make_async_copy(rw1.at[0, pl.ds(0, 2 * KC)], ring.at[slot], ring_sem.at[slot]).wait()

    segments = [(0, N1, first_item, 0), (N1, NA, None, N1), (NA, NB + N1, first_item, NB), (NB + N1, NB + NA, None, NB + N1)]

    def refill(n, low, high):
        for a, b, kind, zero in segments:
            if a >= high or b <= low:
                continue

            def go(kind=kind, zero=zero):
                i = n - zero
                for d in (kind(i, n % NS) if kind else second_item(i // 4, i % 4, n % NS)):
                    d.start()
            if a <= low and high <= b:
                go()
            else:
                pl.when((n >= a) & (n < b))(go)

    def same(ref, sem, dev):
        return remote(ref, ref, sem, dev)

    d_meta = [remote(ids[i], mi.at[1, i], 0, dev_d) for i in range(4)] + [remote(gates[m], mg.at[1, m], 1, dev_d) for m in range(2)]
    d_meta_all = [same(mi.at[1], 0, dev_d), same(mg.at[1], 1, dev_d)]
    x_meta = [remote(ids[i], mi.at[2, i], 2, dev_x) for i in range(4)] + [remote(gates[m], mg.at[2, m], 3, dev_x) for m in range(2)]
    x_meta_all = [same(mi.at[2], 2, dev_x), same(mg.at[2], 3, dev_x)]
    f_meta = [remote(mi.at[2], mi.at[3], 4, dev_d), remote(mg.at[2], mg.at[3], 5, dev_d)]
    d_tok = [remote(toks[m], tok.at[1, m], 6, dev_d) for m in range(2)]
    d_tok_all = same(tok.at[1], 6, dev_d)
    y_tok = [remote(toks[m], ytok.at[pl.ds(m * TOK, TOK)], 7, dev_y) for m in range(2)]
    y_tok_all = same(ytok, 7, dev_y)
    half = part(core, FF // 2)
    y_w2 = remote(sw2.at[half], sw2v.at[1, half], 8, dev_y)
    f_w2 = remote(sw2v.at[1, half], sw2v.at[1, half], 9, dev_d)
    y_hid = remote(buf.at[0, pl.ds(0, 2 * TOK)], hsi, 10, dev_y)
    x_tok, f_tok = [], []
    for k in range(NK):
        cols = part(k, KC)
        x_tok.append([remote(toks[m].at[:, cols], tok.at[2, m, :, cols], 11 + 2 * k + m, dev_x) for m in range(2)])
        f_tok.append([remote(tok.at[2, m, :, cols], tok.at[3, m, :, cols], 11 + 2 * NK + 2 * k + m, dev_d) for m in range(2)])
    base_sem = 11 + 4 * NK
    loc_of = base_sem + 2 * NCH

    def block(kind, m, c):
        return pf.at[m, pl.ds((kind * NCH + c) * TOK, TOK), pl.ds(0, CH)]

    def send_r(m, c):
        return block(0, m, c)

    def send_l(m, c):
        return block(1, m, c)

    def send_x(m, c):
        return block(2, m, c)

    def kept(m, c):
        return block(3, m, c)

    def d_rem(m, c):
        return remote(send_r(m, c), recvr.at[m, :, out_cols(c)], base_sem + 2 * c + m, dev_d)

    def d_loc(m, c):
        return remote(send_l(m, c), recvl.at[m, :, out_cols(c)], loc_of, dev_d)

    d_loc_all = same(recvl, loc_of, dev_d)

    def x_part(m, c):
        to = out_x.at[m] if c == NCH - 1 else xr.at[m, :, out_cols(c)]
        group = 3 if c == NCH - 1 else (0 if m == 0 else max(c - (NCH - 4), 1))
        return remote(send_x(m, c), to, loc_of + 1 + group, dev_x)

    x_part_all = [same(xr.at[0, :, pl.ds(0, (NCH - 1) * CH)], loc_of + 1, dev_x),
                  same(xr.at[1, :, pl.ds(0, (NCH - 2) * CH)], loc_of + 2, dev_x),
                  same(xr.at[1, :, out_cols(NCH - 2)], loc_of + 3, dev_x),
                  same(out_x, loc_of + 4, dev_x)]

    def swiglu(rows, w1, w3):
        p1 = dot(rows, w1)
        p3 = dot(rows, w3)
        return (jax.nn.silu(p1) * p3).astype(BF16)

    def build(src):
        def rows_of(i, _):
            m, b = i // (SROWS // 128), i % (SROWS // 128)
            at = part(b, 128)
            slot = mi[src, 2 * m + 1]
            el = mi[src, 2 * m] - first
            ok = (slot >= 0) & (el >= 0) & (el < NE)
            rid = jnp.where(ok, el * CAP + slot, -1) - b * 128
            g = mg[src, m]
            row = lax.broadcasted_iota(jnp.int32, (128, TOK), 0)
            hit = jnp.zeros((128, TOK), F32)
            gt = jnp.zeros((128, TOK), F32)
            for j in range(TOPK):
                same = row == rid[j:j + 1, :]
                hit = jnp.where(same, 1.0, hit)
                gt = jnp.where(same, g[j:j + 1, :], gt)
            pmat[SRC * m + src, at, :] = hit.astype(BF16)
            gg = gt.T
            hi = jnp.minimum(gg, BF16_MAX).astype(BF16)
            r1 = gg - hi.astype(F32)
            mid = r1.astype(BF16)
            lo = (r1 - mid.astype(F32)).astype(BF16)
            for k, v in enumerate((hi, mid, lo)):
                g3[SRC * m + src, k * TOK:(k + 1) * TOK, at] = v
            return 0
        lax.fori_loop(0, 2 * SROWS // 128, rows_of, 0)

    def dispatch(k, m, pair):
        cols = part(k, KC)
        r0 = dot(pmat[SRC * m + 2 * pair], tok[2 * pair, m, :, cols])
        r1 = dot(pmat[SRC * m + 2 * pair + 1], tok[2 * pair + 1, m, :, cols])
        for e in range(NE):
            both = jnp.concatenate([r0[e * CAP:(e + 1) * CAP], r1[e * CAP:(e + 1) * CAP]], axis=0)
            at = e * ROWS + pair * 2 * CAP
            buf[m, at:at + 2 * CAP, :] = both.astype(BF16)

    def load(ref, ms, at):
        return jnp.concatenate([ref[m, at, :] for m in ms], axis=0) if len(ms) > 1 else ref[ms[0], at, :]

    def stage1(k, ms, half=None):
        per = 4 if len(ms) > 1 else 8
        item0 = k * NE if 0 in ms else NB + k * NE

        def step(i, _):
            for u in range(per):
                wait_item((item0 + per * i + u) % NS)
            for u in range(per):
                e = per * i + u
                slot = (item0 + e) % NS
                rows = load(buf, ms, part(e, ROWS))
                p1 = dot(rows, ring[slot, :KC])
                p3 = dot(rows, ring[slot, KC:])
                at1, at3 = part(2 * e, ROWS), part(2 * e + 1, ROWS)
                if k:
                    p1 = p1 + load(pf, ms, at1)
                    p3 = p3 + load(pf, ms, at3)
                if k == NK - 1:
                    p1 = (jax.nn.silu(p1) * p3).astype(BF16)
                for j, m in enumerate(ms):
                    at = slice(j * ROWS, (j + 1) * ROWS)
                    if k < NK - 1:
                        pf[m, at1, :] = p1[at]
                        pf[m, at3, :] = p3[at]
                    else:
                        hid[m, e] = p1[at]
            for u in range(per):
                low = item0 + NS + (half or 0) * NE // 2
                refill(item0 + per * i + u + NS, low, low + (NE if half is None else NE // 2))
            return 0
        if half is None:
            lax.fori_loop(0, NE // per, step, 0)
        else:
            lax.fori_loop(half * NE // per // 2, (half + 1) * NE // per // 2, step, 0)

    def combine(m, s):
        q = dot(g3[SRC * m + s], buf[m, s * SROWS:(s + 1) * SROWS, :CH])
        return q[:TOK] + q[TOK:2 * TOK] + q[2 * TOK:]

    def stage2(c, m):
        item0 = N1 + c * NE // 4 if m == 0 else NB + N1 + c * NE // 4
        for q in range(NE // 4):
            wait_item((item0 + q) % NS)

        def step(_, unused):
            for q in range(NE // 4):
                r = []
                for e in range(4):
                    a, b = (e // 2) * FF, (e % 2) * CH
                    r.append(dot(hid[m, 4 * q + e], ring[(item0 + q) % NS, a:a + FF, b:b + CH]))
                for s in range(SRC):
                    rows = jnp.concatenate([v[s * CAP:(s + 1) * CAP] for v in r], axis=0)
                    buf[m, s * SROWS + 4 * q * CAP:s * SROWS + 4 * (q + 1) * CAP, :CH] = rows.astype(BF16)
            return 0
        lax.fori_loop(0, 1, step, 0)

        def more(q, _):
            refill(item0 + q + NS, item0 + NS, item0 + NS + NE // 4)
            return 0
        lax.fori_loop(0, NE // 4, more, 0)

    def sums(c, m):
        to_die, to_x = combine(m, 3), combine(m, 2)
        send_r(m, c)[...] = to_die
        d_rem(m, c).start()
        send_x(m, c)[...] = to_x
        to_die, home = combine(m, 1), combine(m, 0)
        send_l(m, c)[...] = to_die
        d_loc(m, c).start()
        kept(m, c)[...] = home

    def pass_on(c, m):
        d_rem(m, c).wait_recv()
        send_x(m, c)[...] = send_x(m, c)[...] + recvr[m, :, c * CH:(c + 1) * CH]
        x_part(m, c).start()

    def arrived(k, ms):
        for m in ms:
            x_tok[k][m].wait_recv()
            f_tok[k][m].start()

    barrier = pltpu.get_barrier_semaphore()
    for dev in (dev_d, dev_x, dev_y):
        pl.semaphore_signal(barrier, inc=1, device_id=dev, device_id_type=MESH)
    for c in own:
        c.start()

    def fill(n, _):
        for c in first_item(n, n):
            c.start()
        return 0
    lax.fori_loop(0, 8, fill, 0)
    pl.semaphore_wait(barrier, 3)
    for c in x_meta + d_meta + x_tok[0] + d_tok + [x_tok[k][m] for m in range(2) for k in range(1, NK)] + y_tok + [y_w2]:
        c.start()
    lax.fori_loop(8, NS, fill, 0)
    for c in own_all:
        c.wait()

    build(0)
    for c in d_meta_all + x_meta_all:
        c.wait_recv()
    for c in f_meta:
        c.start()
    build(1)
    build(2)
    for c in f_meta + [d_tok_all]:
        c.wait_recv()
    build(3)

    both, a, b = (0, 1), (0,), (1,)
    for m in both:
        dispatch(0, m, 0)
    arrived(0, a)
    arrived(0, b)
    for m in both:
        f_tok[0][m].wait_recv()
        dispatch(0, m, 1)
    stage1(0, both, half=0)
    arrived(1, a)
    stage1(0, both, half=1)
    dispatch(1, 0, 0)
    f_tok[1][0].wait_recv()
    dispatch(1, 0, 1)
    stage1(1, a, half=0)
    arrived(2, a)
    stage1(1, a, half=1)
    dispatch(2, 0, 0)
    f_tok[2][0].wait_recv()
    dispatch(2, 0, 1)
    arrived(1, b)
    stage1(2, a)
    for c in range(NCH):
        stage2(c, 0)
        if c:
            pass_on(c - 1, 0)
        sums(c, 0)
        if c == 0:
            dispatch(1, 1, 0)
            f_tok[1][1].wait_recv()
        if c == 2:
            arrived(2, b)
            dispatch(1, 1, 1)

    stage1(1, b)
    pass_on(NCH - 1, 0)
    dispatch(2, 1, 0)
    f_tok[2][1].wait_recv()
    dispatch(2, 1, 1)
    stage1(2, b)
    for c in shared:
        c.start()
    for c in range(NCH):
        stage2(c, 1)
        if c:
            pass_on(c - 1, 1)
        sums(c, 1)
        if c == NCH - 1:
            pass_on(c, 1)
        if c == 3:
            for d in shared:
                d.wait()
            y_tok_all.wait_recv()
            for m in both:
                buf[0, m * TOK:(m + 1) * TOK, :] = swiglu(ytok[m * TOK:(m + 1) * TOK], sw13[0], sw13[1])
            y_hid.start()
    for m in both:
        buf[0, (2 + m) * TOK:(3 + m) * TOK, :] = swiglu(tok[0, m], sw13[0], sw13[1])
    y_w2.wait_recv()
    f_w2.start()
    y_hid.wait_recv()
    d_loc_all.wait_recv()
    f_w2.wait_recv()

    for c in range(NCH - 1, -1, -1):
        at = slice(c * CH, (c + 1) * CH)
        for m in both:
            s = dot(buf[0, (2 + m) * TOK:(3 + m) * TOK, :], sw2v[0, :, at]) + dot(hsi[m * TOK:(m + 1) * TOK, :], sw2v[1, :, at])
            kept(m, c)[...] = kept(m, c)[...] + recvl[m, :, at] + s + tok[0, m, :, at].astype(F32)
            if c == NCH - 1:
                put(m, c).start()
    for m in both:
        for c in range(NCH - 1):
            at = slice(c * CH, (c + 1) * CH)
            if c == 0:
                x_part_all[m].wait_recv()
            if m == 1 and c == NCH - 2:
                x_part_all[2].wait_recv()
            ytok[m * TOK:(m + 1) * TOK, at] = (kept(m, c)[...] + xr[m, :, at]).astype(BF16)
            put(m, c).start()

    for c in x_meta_all + d_meta_all + f_meta + [d_tok_all, y_tok_all, y_w2, f_w2, y_hid, d_loc_all]:
        c.wait_send()
    for c in sum(x_tok, []) + sum(f_tok, []) + x_part_all:
        c.wait_send()
    for c in range(NCH):
        for m in both:
            d_rem(m, c).wait_send()
    local(recvl.at[:, :, out_cols(NCH - 1)], out_kept, 6).wait()
    local(tok.at[0, :, :, pl.ds(0, DIM - CH)], out_ab.at[:, :, pl.ds(0, DIM - CH)], 7).wait()
    x_part_all[3].wait_recv()


def finish(most, kept, x, out_a, out_b, row, k_v, x_v, sem):
    ready = DIM - CH
    early = [pltpu.make_async_copy(most.at[m, :, pl.ds(0, ready)], row.at[m, :, pl.ds(0, ready)], sem.at[m]) for m in range(2)]
    late = [pltpu.make_async_copy(kept.at[m], k_v.at[m], sem.at[2 + m]) for m in range(2)]
    late += [pltpu.make_async_copy(x.at[m], x_v.at[m], sem.at[4 + m]) for m in range(2)]
    for c in late + early:
        c.start()
    for c in late:
        c.wait()
    for m in range(2):
        row[m, :, ready:] = (k_v[m] + x_v[m]).astype(BF16)
    back = []
    for m, out in enumerate((out_a, out_b)):
        early[m].wait()
        back.append(pltpu.make_async_copy(row.at[m], out, sem.at[6 + m]))
        back[m].start()
    for c in back:
        c.wait()


def solution(mesh):
    tok_spec = P(('data', 'ep', 'tp'), None)
    in_specs = (tok_spec,) * 8 + (P(None, 'tp'), P(None, 'tp'), P('tp', None), P('ep', None, None), P('ep', None, None), P('ep', None, None))
    nsem = 11 + 4 * NK + 2 * NCH + 5
    scratch = [
        pltpu.VMEM((NS, 2 * KC, FF), BF16),
        pltpu.VMEM((2, DIM, FF), BF16),
        pltpu.VMEM((2, FF, DIM), BF16),
        pltpu.VMEM((4, 2, TOK, DIM), BF16),
        pltpu.VMEM((2 * TOK, DIM), BF16),
        pltpu.VMEM((2, NE * ROWS, KC), BF16),
        pltpu.VMEM((2, 2 * NE * ROWS, FF), F32),
        pltpu.VMEM((2, NE, ROWS, FF), BF16),
        pltpu.VMEM((2 * SRC, SROWS, TOK), BF16),
        pltpu.VMEM((2 * SRC, 3 * TOK, SROWS), BF16),
        pltpu.VMEM((2, TOK, DIM), F32),
        pltpu.VMEM((2, TOK, DIM), F32),
        pltpu.VMEM((2, TOK, DIM - CH), F32),
        pltpu.VMEM((2 * TOK, FF), BF16),
        pltpu.VMEM((4, 4, TOPK, TOK), jnp.int32),
        pltpu.VMEM((4, 2, TOPK, TOK), F32),
        pltpu.SemaphoreType.DMA((8,)),
        pltpu.SemaphoreType.DMA((NS,)),
        pltpu.SemaphoreType.DMA((nsem,)),
        pltpu.SemaphoreType.DMA((nsem,)),
    ]

    def layer_local(tokens_a, tokens_b, experts_a, experts_b, gates_a, gates_b, slots_a, slots_b, shared_w1, shared_w3, shared_w2, routed_w1, routed_w3, routed_w2):
        hbm = pl.BlockSpec(memory_space=pl.ANY)
        tail = jax.ShapeDtypeStruct((2, TOK, CH), F32)
        parts = pl.pallas_call(
            kernel,
            out_shape=(jax.ShapeDtypeStruct((2, TOK, DIM), BF16), tail, tail),
            in_specs=[hbm] * 14,
            out_specs=(hbm,) * 3,
            scratch_shapes=scratch,
            compiler_params=pltpu.CompilerParams(collective_id=0, has_side_effects=True, vmem_limit_bytes=67043328),
        )(tokens_a, tokens_b, experts_a.T, slots_a.T, experts_b.T, slots_b.T, gates_a.T, gates_b.T,
          shared_w1, shared_w3, shared_w2, routed_w1, routed_w3, routed_w2)
        return pl.pallas_call(
            finish,
            out_shape=(jax.ShapeDtypeStruct((TOK, DIM), BF16),) * 2,
            in_specs=[hbm] * 3,
            out_specs=(hbm,) * 2,
            scratch_shapes=[pltpu.VMEM((2, TOK, DIM), BF16), pltpu.VMEM((2, TOK, CH), F32),
                            pltpu.VMEM((2, TOK, CH), F32), pltpu.SemaphoreType.DMA((8,))],
        )(*parts)

    return jax.shard_map(layer_local, mesh=mesh, in_specs=in_specs, out_specs=(tok_spec, tok_spec), check_vma=False)
```

```python
import functools

import jax
import jax.numpy as jnp
from jax import lax
from jax.experimental import pallas as pl
from jax.experimental.pallas import tpu as pltpu
from jax.sharding import PartitionSpec as P

MESH = pl.DeviceIdType.MESH
F32, BF16 = jnp.float32, jnp.bfloat16

TOK = 128
DIM = 1536
FF = 512
TOPK = 6
CAP = 24
NE = 16
SRC = 4
ROWS = SRC * CAP
SROWS = NE * CAP
KC = 512
NK = DIM // KC
CH = 256
NCH = DIM // CH
NS = 24
N1 = NK * NE
N2 = NCH * NE // 4
NA = N1 + N2
NB = NA - NE
BF16_MAX = 3.3895313892515355e38


def dot(a, b):
    return jnp.dot(a, b, preferred_element_type=F32)


def kernel(tok_a, tok_b, e_a, s_a, e_b, s_b, g_a, g_b, sw1, sw3, sw2, rw1, rw3, rw2,
           out_ab, out_kept, out_x,
           ring, sw13, sw2v, tok, ytok, buf, pf, hid, g3,
           recvr, recvl, xr, hsi, mi, mg,
           loc_sem, ring_sem, snd, rcv):
    tp = lax.axis_index('tp')
    ep = lax.axis_index('ep')
    core = lax.rem(ep, 2)
    first = ep * NE
    dev_d = {'ep': ep + 1 - 2 * core}
    dev_x = {'ep': lax.rem(ep + 2, 4)}
    dev_y = {'tp': 1 - tp}
    toks, ids, gates = (tok_a, tok_b), (e_a, s_a, e_b, s_b), (g_a, g_b)

    def local(src, dst, sem):
        return pltpu.make_async_copy(src, dst, loc_sem.at[sem])

    def remote(src, dst, sem, dev, kind):
        return pltpu.make_async_remote_copy(src_ref=src, dst_ref=dst, send_sem=snd.at[kind], recv_sem=rcv.at[sem],
                                            device_id=dev, device_id_type=MESH)

    def mult(i, k):
        return i * k if isinstance(i, int) else pl.multiple_of(i * k, k)

    def part(i, k):
        return pl.ds(mult(i, k), k)

    own = [local(ids[i], mi.at[0, i], 0) for i in range(4)] + [local(gates[m], mg.at[0, m], 1) for m in range(2)]
    own += [local(toks[m], tok.at[0, m], 2) for m in range(2)]
    own_all = [local(mi.at[1], mi.at[0], 0), local(mg.at[1], mg.at[0], 1), local(tok.at[1], tok.at[0], 2)]
    shared = [local(sw1, sw13.at[0], 3), local(sw3, sw13.at[1], 4), local(sw2, sw2v.at[0], 5)]

    def out_cols(c):
        return part(c, CH)

    def put(m, c):
        if c == NCH - 1:
            return local(kept(m, c), out_kept.at[m], 6)
        return local(ytok.at[part(m, TOK), out_cols(c)], out_ab.at[m, :, out_cols(c)], 7)

    def first_item(n, slot):
        e, rows = n % NE, part(n // NE, KC)
        return (pltpu.make_async_copy(rw1.at[e, rows], ring.at[slot, pl.ds(0, KC)], ring_sem.at[slot // 4]),
                pltpu.make_async_copy(rw3.at[e, rows], ring.at[slot, pl.ds(KC, KC)], ring_sem.at[slot // 4]))

    def second_item(c, q, slot):
        return [pltpu.make_async_copy(rw2.at[4 * q + i, :, out_cols(c)],
                                      ring.at[slot, pl.ds((i // 2) * FF, FF), pl.ds((i % 2) * CH, CH)],
                                      ring_sem.at[slot // 4]) for i in range(4)]

    def wait_items(n):
        slot = n % NS
        pltpu.make_async_copy(rw1.at[pl.ds(0, 4), pl.ds(0, 2 * KC)], ring.at[part(slot // 4, 4)], ring_sem.at[slot // 4]).wait()

    segments = [(0, N1, first_item, 0), (N1, NA, None, N1), (NA, NB + N1, first_item, NB), (NB + N1, NB + NA, None, NB + N1)]

    def refill(n, low, high):
        for a, b, kind, zero in segments:
            if a >= high or b <= low:
                continue

            def go(kind=kind, zero=zero):
                i = n - zero
                for d in (kind(i, n % NS) if kind else second_item(i // 4, i % 4, n % NS)):
                    d.start()
            if a <= low and high <= b:
                go()
            else:
                pl.when((n >= a) & (n < b))(go)

    def same(ref, sem, dev, kind):
        return remote(ref, ref, sem, dev, kind)

    d_meta = [remote(ids[i], mi.at[1, i], 0, dev_d, 1) for i in range(4)] + [remote(gates[m], mg.at[1, m], 1, dev_d, 2) for m in range(2)]
    d_meta_all = [same(mi.at[1], 0, dev_d, 1), same(mg.at[1], 1, dev_d, 2)]
    x_meta = [remote(ids[i], mi.at[2, i], 2, dev_x, 1) for i in range(4)] + [remote(gates[m], mg.at[2, m], 3, dev_x, 2) for m in range(2)]
    x_meta_all = [same(mi.at[2], 2, dev_x, 1), same(mg.at[2], 3, dev_x, 2)]
    f_meta = [remote(mi.at[2], mi.at[3], 4, dev_d, 1), remote(mg.at[2], mg.at[3], 5, dev_d, 2)]
    d_tok = [remote(toks[m], tok.at[1, m], 6, dev_d, 0) for m in range(2)]
    d_tok_all = same(tok.at[1], 6, dev_d, 0)
    y_tok = [remote(toks[m], ytok.at[pl.ds(m * TOK, TOK)], 7, dev_y, 0) for m in range(2)]
    y_tok_all = same(ytok, 7, dev_y, 0)
    half = part(core, FF // 2)
    y_w2 = remote(sw2.at[half], sw2v.at[1, half], 8, dev_y, 3)
    f_w2 = remote(sw2v.at[1, half], sw2v.at[1, half], 9, dev_d, 3)
    y_hid = remote(buf.at[0, pl.ds(0, 2 * TOK)], hsi, 10, dev_y, 4)
    x_tok, f_tok = [], []
    for k in range(NK):
        cols = part(k, KC)
        x_tok.append([remote(toks[m].at[:, cols], tok.at[2, m, :, cols], 11 + 2 * k + m, dev_x, 0) for m in range(2)])
        f_tok.append([remote(tok.at[2, m, :, cols], tok.at[3, m, :, cols], 11 + 2 * NK + 2 * k + m, dev_d, 0) for m in range(2)])
    base_sem = 11 + 4 * NK
    loc_of = base_sem + 2 * NCH

    def block(kind, m, c):
        return pf.at[m, pl.ds((kind * NCH + c) * TOK, TOK), pl.ds(0, CH)]

    def send_r(m, c):
        return block(0, m, c)

    def send_l(m, c):
        return block(1, m, c)

    def send_x(m, c):
        return block(2, m, c)

    def kept(m, c):
        return block(3, m, c)

    def d_rem(m, c):
        return remote(send_r(m, c), recvr.at[m, :, out_cols(c)], base_sem + 2 * c + m, dev_d, 5)

    def d_loc(m, c):
        return remote(send_l(m, c), recvl.at[m, :, out_cols(c)], loc_of, dev_d, 6)

    d_loc_all = same(recvl, loc_of, dev_d, 6)

    def x_part(m, c):
        to = out_x.at[m] if c == NCH - 1 else xr.at[m, :, out_cols(c)]
        group = 3 if c == NCH - 1 else (0 if m == 0 else max(c - (NCH - 4), 1))
        return remote(send_x(m, c), to, loc_of + 1 + group, dev_x, 7)

    x_part_all = [same(xr.at[0, :, pl.ds(0, (NCH - 1) * CH)], loc_of + 1, dev_x, 7),
                  same(xr.at[1, :, pl.ds(0, (NCH - 2) * CH)], loc_of + 2, dev_x, 7),
                  same(xr.at[1, :, out_cols(NCH - 2)], loc_of + 3, dev_x, 7),
                  same(out_x, loc_of + 4, dev_x, 7)]

    def swiglu(rows, w1, w3):
        p1 = dot(rows, w1)
        p3 = dot(rows, w3)
        return (jax.nn.silu(p1) * p3).astype(BF16)

    def build(src):
        def rows_of(i, _):
            m, b = i // (SROWS // 128), i % (SROWS // 128)
            at = part(b, 128)
            slot = mi[src, 2 * m + 1]
            el = mi[src, 2 * m] - first
            ok = (slot >= 0) & (el >= 0) & (el < NE)
            rid = jnp.where(ok, el * CAP + slot, -1) - b * 128
            g = mg[src, m]
            row = lax.broadcasted_iota(jnp.int32, (128, TOK), 0)
            hit = jnp.zeros((128, TOK), F32)
            gt = jnp.zeros((128, TOK), F32)
            for j in range(TOPK):
                same = row == rid[j:j + 1, :]
                hit = jnp.where(same, 1.0, hit)
                gt = jnp.where(same, g[j:j + 1, :], gt)
            hid[1, part(src * (SROWS // 128) + b, 128), part(m, TOK)] = hit.astype(BF16)
            gg = gt.T
            hi = jnp.minimum(gg, BF16_MAX).astype(BF16)
            r1 = gg - hi.astype(F32)
            mid = r1.astype(BF16)
            lo = (r1 - mid.astype(F32)).astype(BF16)
            for k, v in enumerate((hi, mid, lo)):
                g3[SRC * m + src, k * TOK:(k + 1) * TOK, at] = v
            return 0
        lax.fori_loop(0, 2 * SROWS // 128, rows_of, 0)

    def dispatch(k, m, pair):
        cols = part(k, KC)
        place = [hid[1, s * SROWS:(s + 1) * SROWS, m * TOK:(m + 1) * TOK] for s in (2 * pair, 2 * pair + 1)]
        r0 = dot(place[0], tok[2 * pair, m, :, cols])
        r1 = dot(place[1], tok[2 * pair + 1, m, :, cols])
        for e in range(NE):
            both = jnp.concatenate([r0[e * CAP:(e + 1) * CAP], r1[e * CAP:(e + 1) * CAP]], axis=0)
            at = e * ROWS + pair * 2 * CAP
            buf[m, at:at + 2 * CAP, :] = both.astype(BF16)

    def load(ref, ms, at):
        return jnp.concatenate([ref[m, at, :] for m in ms], axis=0) if len(ms) > 1 else ref[ms[0], at, :]

    def stage1(k, ms, half=None):
        per = 8
        item0 = k * NE if 0 in ms else NB + k * NE

        def step(i, _):
            for u in range(0, per, 4):
                wait_items(item0 + per * i + u)
            for u in range(per):
                e = per * i + u
                slot = (item0 + e) % NS
                rows = load(buf, ms, part(e, ROWS))
                p1 = dot(rows, ring[slot, :KC])
                p3 = dot(rows, ring[slot, KC:])
                at1, at3 = part(2 * e, ROWS), part(2 * e + 1, ROWS)
                if k:
                    p1 = p1 + load(pf, ms, at1)
                    p3 = p3 + load(pf, ms, at3)
                if k == NK - 1:
                    p1 = (jax.nn.silu(p1) * p3).astype(BF16)
                for j, m in enumerate(ms):
                    at = slice(j * ROWS, (j + 1) * ROWS)
                    if k < NK - 1:
                        pf[m, at1, :] = p1[at]
                        pf[m, at3, :] = p3[at]
                    else:
                        hid[m, part(e, ROWS), :] = p1[at]
            for u in range(per):
                low = item0 + NS + (half or 0) * NE // 2
                refill(item0 + per * i + u + NS, low, low + (NE if half is None else NE // 2))
            return 0
        if half is None:
            lax.fori_loop(0, NE // per, step, 0)
        else:
            lax.fori_loop(half * NE // per // 2, (half + 1) * NE // per // 2, step, 0)

    def combine(m, s):
        q = dot(g3[SRC * m + s], buf[m, s * SROWS:(s + 1) * SROWS, :CH])
        return q[:TOK] + q[TOK:2 * TOK] + q[2 * TOK:]

    def stage2(c, m):
        item0 = N1 + c * NE // 4 if m == 0 else NB + N1 + c * NE // 4
        wait_items(item0)

        def step(_, unused):
            for q in range(NE // 4):
                r = []
                for e in range(4):
                    a, b = (e // 2) * FF, (e % 2) * CH
                    r.append(dot(hid[m, part(4 * q + e, ROWS), :], ring[(item0 + q) % NS, a:a + FF, b:b + CH]))
                for s in range(SRC):
                    rows = jnp.concatenate([v[s * CAP:(s + 1) * CAP] for v in r], axis=0)
                    buf[m, s * SROWS + 4 * q * CAP:s * SROWS + 4 * (q + 1) * CAP, :CH] = rows.astype(BF16)
            return 0
        lax.fori_loop(0, 1, step, 0)

        def more(q, _):
            refill(item0 + q + NS, item0 + NS, item0 + NS + NE // 4)
            return 0
        lax.fori_loop(0, NE // 4, more, 0)

    def sums(c, m):
        to_die, to_x = combine(m, 3), combine(m, 2)
        if c:
            die_own, home = combine(m, 1), combine(m, 0)
        send_r(m, c)[...] = to_die
        d_rem(m, c).start()
        send_x(m, c)[...] = to_x
        if not c:
            die_own, home = combine(m, 1), combine(m, 0)
        send_l(m, c)[...] = die_own
        d_loc(m, c).start()
        kept(m, c)[...] = home

    def pass_on(c, m):
        d_rem(m, c).wait_recv()
        send_x(m, c)[...] = send_x(m, c)[...] + recvr[m, :, c * CH:(c + 1) * CH]
        x_part(m, c).start()

    def arrived(k, ms):
        for m in ms:
            x_tok[k][m].wait_recv()
            f_tok[k][m].start()

    barrier = pltpu.get_barrier_semaphore()
    for dev in (dev_d, dev_x, dev_y):
        pl.semaphore_signal(barrier, inc=1, device_id=dev, device_id_type=MESH)
    for c in own:
        c.start()

    def fill(n, _):
        for c in first_item(n, n):
            c.start()
        return 0
    lax.fori_loop(0, 8, fill, 0)
    pl.semaphore_wait(barrier, 3)
    for c in x_meta + d_meta + x_tok[0] + d_tok + [x_tok[k][m] for m in range(2) for k in range(1, NK)] + y_tok + [y_w2]:
        c.start()
    lax.fori_loop(8, NS, fill, 0)
    for c in own_all:
        c.wait()

    build(0)
    for c in d_meta_all + x_meta_all:
        c.wait_recv()
    for c in f_meta:
        c.start()
    build(1)
    build(2)
    for c in f_meta + [d_tok_all]:
        c.wait_recv()
    build(3)

    both, a, b = (0, 1), (0,), (1,)
    for m in both:
        dispatch(0, m, 0)
    arrived(0, a)
    arrived(0, b)
    for m in both:
        f_tok[0][m].wait_recv()
        dispatch(0, m, 1)
    stage1(0, both, half=0)
    arrived(1, a)
    stage1(0, both, half=1)
    dispatch(1, 0, 0)
    f_tok[1][0].wait_recv()
    dispatch(1, 0, 1)
    stage1(1, a, half=0)
    arrived(2, a)
    stage1(1, a, half=1)
    dispatch(2, 0, 0)
    f_tok[2][0].wait_recv()
    dispatch(2, 0, 1)
    arrived(1, b)
    stage1(2, a)
    for c in range(NCH):
        stage2(c, 0)
        if c:
            pass_on(c - 1, 0)
        sums(c, 0)
        if c == 0:
            dispatch(1, 1, 0)
            f_tok[1][1].wait_recv()
        if c == 2:
            arrived(2, b)
            dispatch(1, 1, 1)

    stage1(1, b)
    pass_on(NCH - 1, 0)
    dispatch(2, 1, 0)
    f_tok[2][1].wait_recv()
    dispatch(2, 1, 1)
    stage1(2, b)
    for c in shared:
        c.start()
    for c in range(NCH):
        stage2(c, 1)
        if c:
            pass_on(c - 1, 1)
        sums(c, 1)
        if c == NCH - 1:
            pass_on(c, 1)
        if c == 3:
            for d in shared:
                d.wait()
            y_tok_all.wait_recv()
            for m in both:
                buf[0, m * TOK:(m + 1) * TOK, :] = swiglu(ytok[m * TOK:(m + 1) * TOK], sw13[0], sw13[1])
            y_hid.start()
    for m in both:
        buf[0, (2 + m) * TOK:(3 + m) * TOK, :] = swiglu(tok[0, m], sw13[0], sw13[1])
    y_w2.wait_recv()
    f_w2.start()
    y_hid.wait_recv()
    d_loc_all.wait_recv()
    f_w2.wait_recv()

    for c in range(NCH - 1, -1, -1):
        at = slice(c * CH, (c + 1) * CH)
        for m in both:
            s = dot(buf[0, (2 + m) * TOK:(3 + m) * TOK, :], sw2v[0, :, at]) + dot(hsi[m * TOK:(m + 1) * TOK, :], sw2v[1, :, at])
            kept(m, c)[...] = kept(m, c)[...] + recvl[m, :, at] + s + tok[0, m, :, at].astype(F32)
            if c == NCH - 1:
                put(m, c).start()
    for m in both:
        for c in range(NCH - 1):
            at = slice(c * CH, (c + 1) * CH)
            if c == 0:
                x_part_all[m].wait_recv()
            if m == 1 and c == NCH - 2:
                x_part_all[2].wait_recv()
            ytok[m * TOK:(m + 1) * TOK, at] = (kept(m, c)[...] + xr[m, :, at]).astype(BF16)
            put(m, c).start()

    for kind, ref in enumerate((tok, mi.at[pl.ds(0, 3)], mg.at[pl.ds(0, 3)], sw2v.at[1], hsi, recvr, recvl, recvr)):
        same(ref, 0, dev_d, kind).wait_send()
    local(recvl.at[:, :, out_cols(NCH - 1)], out_kept, 6).wait()
    local(tok.at[0, :, :, pl.ds(0, DIM - CH)], out_ab.at[:, :, pl.ds(0, DIM - CH)], 7).wait()
    x_part_all[3].wait_recv()


def finish(most, kept, x, out_a, out_b, row, k_v, x_v, sem):
    ready = DIM - CH
    early = [pltpu.make_async_copy(most.at[m, :, pl.ds(0, ready)], row.at[m, :, pl.ds(0, ready)], sem.at[m]) for m in range(2)]
    late = [pltpu.make_async_copy(kept.at[m], k_v.at[m], sem.at[2 + m]) for m in range(2)]
    late += [pltpu.make_async_copy(x.at[m], x_v.at[m], sem.at[4 + m]) for m in range(2)]
    for c in late + early:
        c.start()
    for c in late:
        c.wait()
    for m in range(2):
        row[m, :, ready:] = (k_v[m] + x_v[m]).astype(BF16)
    back = []
    for m, out in enumerate((out_a, out_b)):
        early[m].wait()
        back.append(pltpu.make_async_copy(row.at[m], out, sem.at[6 + m]))
        back[m].start()
    for c in back:
        c.wait()


def solution(mesh):
    tok_spec = P(('data', 'ep', 'tp'), None)
    in_specs = (tok_spec,) * 8 + (P(None, 'tp'), P(None, 'tp'), P('tp', None), P('ep', None, None), P('ep', None, None), P('ep', None, None))
    nsem = 11 + 4 * NK + 2 * NCH + 5
    scratch = [
        pltpu.VMEM((NS, 2 * KC, FF), BF16),
        pltpu.VMEM((2, DIM, FF), BF16),
        pltpu.VMEM((2, FF, DIM), BF16),
        pltpu.VMEM((4, 2, TOK, DIM), BF16),
        pltpu.VMEM((2 * TOK, DIM), BF16),
        pltpu.VMEM((2, NE * ROWS, KC), BF16),
        pltpu.VMEM((2, 2 * NE * ROWS, FF), F32),
        pltpu.VMEM((2, NE * ROWS, FF), BF16),
        pltpu.VMEM((2 * SRC, 3 * TOK, SROWS), BF16),
        pltpu.VMEM((2, TOK, DIM), F32),
        pltpu.VMEM((2, TOK, DIM), F32),
        pltpu.VMEM((2, TOK, DIM - CH), F32),
        pltpu.VMEM((2 * TOK, FF), BF16),
        pltpu.VMEM((4, 4, TOPK, TOK), jnp.int32),
        pltpu.VMEM((4, 2, TOPK, TOK), F32),
        pltpu.SemaphoreType.DMA((8,)),
        pltpu.SemaphoreType.DMA((NS // 4,)),
        pltpu.SemaphoreType.DMA((8,)),
        pltpu.SemaphoreType.DMA((nsem,)),
    ]

    def layer_local(tokens_a, tokens_b, experts_a, experts_b, gates_a, gates_b, slots_a, slots_b, shared_w1, shared_w3, shared_w2, routed_w1, routed_w3, routed_w2):
        hbm = pl.BlockSpec(memory_space=pl.ANY)
        tail = jax.ShapeDtypeStruct((2, TOK, CH), F32)
        parts = pl.pallas_call(
            kernel,
            out_shape=(jax.ShapeDtypeStruct((2, TOK, DIM), BF16), tail, tail),
            in_specs=[hbm] * 14,
            out_specs=(hbm,) * 3,
            scratch_shapes=scratch,
            compiler_params=pltpu.CompilerParams(collective_id=0, has_side_effects=True, vmem_limit_bytes=67043328),
        )(tokens_a, tokens_b, experts_a.T, slots_a.T, experts_b.T, slots_b.T, gates_a.T, gates_b.T,
          shared_w1, shared_w3, shared_w2, routed_w1, routed_w3, routed_w2)
        return pl.pallas_call(
            finish,
            out_shape=(jax.ShapeDtypeStruct((TOK, DIM), BF16),) * 2,
            in_specs=[hbm] * 3,
            out_specs=(hbm,) * 2,
            scratch_shapes=[pltpu.VMEM((2, TOK, DIM), BF16), pltpu.VMEM((2, TOK, CH), F32),
                            pltpu.VMEM((2, TOK, CH), F32), pltpu.SemaphoreType.DMA((8,))],
        )(*parts)

    return jax.shard_map(layer_local, mesh=mesh, in_specs=in_specs, out_specs=(tok_spec, tok_spec), check_vma=False)
```
